32 devices in a mesh: ta: 8 (over y, x, core), gz: 4 (over z).
Axes of the slice: x: 2, y: 2, z: 4, core: 2. Of those that a mesh axis runs over, the one named last changes fastest.
Arguments:
- spinor: float32 [2, 4, 3, 16, 8, 768], P(None, None, None, 'ta', 'gz'), may hold values from -3 to 3
- links: float32 [4, 2, 3, 3, 16, 8, 768], P(None, None, None, None, 'ta', 'gz'), may hold values from -3.5 to 3.5
- clover: float32 [2, 2, 6, 6, 16, 8, 768], P(None, None, None, None, 'ta', 'gz'), may hold values from -1.2 to 1.2
Outputs:
- applied: float32 [2, 4, 3, 16, 8, 768], P(None, None, None, 'ta', 'gz')
- force: float32 [4, 2, 3, 3, 16, 8, 768], P(None, None, None, None, 'ta', 'gz')
The draws below stay inside these ranges and needn't reach their ends.
All inputs are finite; a program needn't handle non-finite values.
Results may differ from the reference program's by a relative error of at most 0.0001.
Values sent between devices are 32-bit elements; how exact they have to be, the bound alone decides.
A program may use at most 64 MiB of HBM per device.

```python
import jax
import jax.numpy as jnp

NY = 12
NX = 64
PLANE = 768
NT = 16
NZ = 8


def shard_levels(stream_key, extent, pieces, least, largest):
    def one(dim, shards_of):
        heights = jax.random.uniform(jax.random.fold_in(jax.random.fold_in(stream_key, 6), dim), (shards_of,), jnp.float32, least / len(pieces), largest / len(pieces))
        return jnp.repeat(jnp.exp(heights), extent[dim] // shards_of).reshape((-1,) + (1,) * (len(extent) - dim - 1))

    gain = one(*pieces[0])
    for cut in pieces[1:]:
        gain = gain * one(*cut)
    return gain


def centred(key, extent, spread, limit, shards=(), kind=jnp.bfloat16):
    array = jax.random.normal(key, extent, jnp.float32) * spread
    if len(shards) > 0:
        array = shard_levels(key, extent, shards, -0.22, 0.18) * array
    return jnp.clip(array, min=-limit, max=limit).astype(kind)


def setup_inputs(seed: int = 0) -> dict:
    key_of = jax.random.split(jax.random.key(seed), 4)
    spinor = centred(key_of[0], (2, 4, 3, NT, NZ, PLANE), 0.5, 3.0, ((3, 8), (4, 4)), jnp.float32)
    links = centred(key_of[1], (4, 2, 3, 3, NT, NZ, PLANE), 3 ** -0.5, 3.5, ((4, 8), (5, 4)), jnp.float32)
    clover = centred(key_of[2], (2, 2, 6, 6, NT, NZ, PLANE), 0.2, 1.2, ((4, 8), (5, 4)), jnp.float32)
    return {"spinor": spinor, "links": links, "clover": clover}


bare_mass = -0.25

gamma_table = (
    ((3, 0.0, -1.0), (2, 0.0, -1.0), (1, 0.0, 1.0), (0, 0.0, 1.0)),
    ((3, -1.0, 0.0), (2, 1.0, 0.0), (1, 1.0, 0.0), (0, -1.0, 0.0)),
    ((2, 0.0, -1.0), (3, 0.0, 1.0), (0, 0.0, 1.0), (1, 0.0, -1.0)),
    ((2, 1.0, 0.0), (3, 1.0, 0.0), (0, 1.0, 0.0), (1, 1.0, 0.0)),
)


def apply_gamma(hop_dir, field):
    parts_re = []
    parts_im = []
    for spin_row in range(4):
        source, phase_re, phase_im = gamma_table[hop_dir][spin_row]
        source_re = field[0, source]
        source_im = field[1, source]
        if phase_im == 0.0:
            parts_re.append(phase_re * source_re)
            parts_im.append(phase_re * source_im)
        else:
            parts_re.append(-phase_im * source_im)
            parts_im.append(phase_im * source_re)
    return jnp.stack([jnp.stack(parts_re), jnp.stack(parts_im)])


def project(hop_dir, field, sign):
    return field + sign * apply_gamma(hop_dir, field)


def color_apply(link, field, dagger):
    link_re = link[0]
    link_im = link[1]
    if dagger:
        link_re = jnp.swapaxes(link_re, 0, 1)
        link_im = -jnp.swapaxes(link_im, 0, 1)
    matrix_re = link_re[None]
    matrix_im = link_im[None]
    field_re = field[0][:, None]
    field_im = field[1][:, None]
    out_re = jnp.sum(matrix_re * field_re - matrix_im * field_im, axis=2)
    out_im = jnp.sum(matrix_re * field_im + matrix_im * field_re, axis=2)
    return jnp.stack([out_re, out_im])


def clover_apply(clover, field):
    halves = field.reshape((2, 2, 6) + field.shape[3:])
    field_re = halves[0][:, None]
    field_im = halves[1][:, None]
    out_re = jnp.sum(clover[0] * field_re - clover[1] * field_im, axis=2)
    out_im = jnp.sum(clover[0] * field_im + clover[1] * field_re, axis=2)
    return jnp.stack([out_re, out_im]).reshape(field.shape)


def spin_outer(left, right):
    left_re = left[0][:, :, None]
    left_im = left[1][:, :, None]
    right_re = right[0][:, None]
    right_im = right[1][:, None]
    out_re = jnp.sum(left_re * right_re + left_im * right_im, axis=0)
    out_im = jnp.sum(left_im * right_re - left_re * right_im, axis=0)
    return jnp.stack([out_re, out_im])


def color_product(first, second):
    first_re = first[0][:, :, None]
    first_im = first[1][:, :, None]
    second_re = second[0][None]
    second_im = second[1][None]
    out_re = jnp.sum(first_re * second_re - first_im * second_im, axis=1)
    out_im = jnp.sum(first_re * second_im + first_im * second_re, axis=1)
    return jnp.stack([out_re, out_im])


def traceless(matrix):
    mat_re = matrix[0]
    mat_im = matrix[1]
    anti_re = 0.5 * (mat_re - jnp.swapaxes(mat_re, 0, 1))
    anti_im = 0.5 * (mat_im + jnp.swapaxes(mat_im, 0, 1))
    trace_third = (mat_im[0, 0] + mat_im[1, 1] + mat_im[2, 2]) / 3.0
    identity = jnp.eye(3, dtype=jnp.float32).reshape((3, 3) + (1,) * (mat_re.ndim - 2))
    return jnp.stack([anti_re, anti_im - identity * trace_third])


def along_plane(field, hop_dir, step):
    shape = field.shape
    grid = field.reshape(shape[:-1] + (NY, NX))
    if hop_dir == 0:
        grid = jnp.roll(grid, -step, axis=-1)
    else:
        grid = jnp.roll(grid, -step, axis=-2)
    return grid.reshape(shape)


def neighbor(field, hop_dir, step, fermion):
    if hop_dir < 2:
        return along_plane(field, hop_dir, step)
    if hop_dir == 2:
        return jnp.roll(field, -step, axis=4)
    moved = jnp.roll(field, -step, axis=3)
    if fermion:
        boundary = field.shape[3] - 1 if step == 1 else 0
        moved = moved.at[:, :, :, boundary].multiply(-1.0)
    return moved


def reference(spinor, links, clover):
    hopping = jnp.zeros_like(spinor)
    forward_half = []
    for hop_dir in range(4):
        ahead_proj = project(hop_dir, neighbor(spinor, hop_dir, 1, True), -1.0)
        forward_half.append(ahead_proj)
        behind = neighbor(spinor, hop_dir, -1, True)
        back_link = neighbor(links[hop_dir], hop_dir, -1, False)
        hopping = hopping + color_apply(links[hop_dir], ahead_proj, False) + color_apply(back_link, project(hop_dir, behind, 1.0), True)
    applied = (4.0 + bare_mass) * spinor + clover_apply(clover, spinor) - 0.5 * hopping
    forces = []
    for hop_dir in range(4):
        ahead_applied = neighbor(applied, hop_dir, 1, True)
        summed = spin_outer(forward_half[hop_dir], applied) + spin_outer(project(hop_dir, ahead_applied, 1.0), spinor)
        forces.append(traceless(color_product(links[hop_dir], summed)))
    return applied, jnp.stack(forces)
```

```python
import jax
import jax.numpy as jnp
from jax import lax
from jax.experimental import pallas as pl
from jax.experimental.pallas import tpu as pltpu
from jax.sharding import PartitionSpec as P

NX = 64
LANES = 128
TILE = 8
MESH = pl.DeviceIdType.MESH

bare_mass = -0.25
gamma_table = (
    ((3, 0.0, -1.0), (2, 0.0, -1.0), (1, 0.0, 1.0), (0, 0.0, 1.0)),
    ((3, -1.0, 0.0), (2, 1.0, 0.0), (1, 1.0, 0.0), (0, -1.0, 0.0)),
    ((2, 0.0, -1.0), (3, 0.0, 1.0), (0, 0.0, 1.0), (1, 0.0, -1.0)),
    ((2, 1.0, 0.0), (3, 1.0, 0.0), (0, 1.0, 0.0), (1, 1.0, 0.0)),
)


def add_signed(a, b, positive):
    return a + b if positive else a - b


def add_phase(a, b, phase_re, phase_im):
    if phase_im == 0.0:
        up = phase_re > 0
        return (add_signed(a[0], b[0], up), add_signed(a[1], b[1], up))
    up = phase_im > 0
    return (add_signed(a[0], b[1], not up), add_signed(a[1], b[0], up))


def half(mu, field, sign):
    out = []
    for s in range(2):
        source, p_re, p_im = gamma_table[mu][s]
        out.append(
            [add_phase(field[s][c], field[source][c], sign * p_re, sign * p_im) for c in range(3)]
        )
    return out


def add_whole(mu, total, halves, sign):
    out = [[add_phase(total[s][c], halves[s][c], 1.0, 0.0) for c in range(3)] for s in range(2)]
    for s in (2, 3):
        source, p_re, p_im = gamma_table[mu][s]
        out.append(
            [add_phase(total[s][c], halves[source][c], sign * p_re, sign * p_im) for c in range(3)]
        )
    return out


def csum(terms):
    total = terms[0]
    for term in terms[1:]:
        total = total + term
    return total


def mat_vec(link, vec, dagger):
    out = []
    for s in range(2):
        rows = []
        for a in range(3):
            re, im = [], []
            for b in range(3):
                h = vec[s][b]
                if dagger:
                    m = link[b][a]
                    re.append(m[0] * h[0] + m[1] * h[1])
                    im.append(m[0] * h[1] - m[1] * h[0])
                else:
                    m = link[a][b]
                    re.append(m[0] * h[0] - m[1] * h[1])
                    im.append(m[0] * h[1] + m[1] * h[0])
            rows.append((csum(re), csum(im)))
        out.append(rows)
    return out


def flat(ref):
    return ref.reshape(ref.shape[0], ref.shape[1] * ref.shape[2], ref.shape[3])


def parts_of(whole, held):
    parts = whole.shape[-1] // LANES
    for t in range(whole.shape[-3]):
        for q in range(parts):
            yield whole.at[:, t, :, pl.ds(LANES * q, LANES)], held.at[:, parts * t + q]


def write_out(phi_ref, force_ref, out_hbm, force_hbm, sem):
    for n, (whole, held) in enumerate(((force_hbm, force_ref), (out_hbm, phi_ref))):
        for dst, src in parts_of(whole, held):
            pltpu.make_async_copy(src, dst, sem.at[n]).start()
    for n, held in enumerate((force_ref, phi_ref)):
        pltpu.make_async_copy(held, held, sem.at[n]).wait()


def kernel(nt, nz, x_hbm, u_hbm, c_hbm, phi_out, force_out, psi_in, link_in, clov_in, hm, hp, bl,
           sh_hm, sh_bl, prod, acc, hphi, sh_hphi, face_out, face_in, in_sem, send_sem, recv_sem):
    psi, link, clov, out_ref, force_ref = map(flat, (psi_in, link_in, clov_in, phi_out, force_out))
    rows = psi.shape[1]
    face_t = rows // nt
    face_z = rows // nz
    chunks = rows // TILE
    t_place, z_place = lax.axis_index("ta"), lax.axis_index("gz")
    t_count, z_count = lax.axis_size("ta"), lax.axis_size("gz")
    t_next = (lax.rem(t_place + 1, t_count), z_place)
    t_prev = (lax.rem(t_place + t_count - 1, t_count), z_place)
    z_next = (t_place, lax.rem(z_place + 1, z_count))
    z_prev = (t_place, lax.rem(z_place + z_count - 1, z_count))
    low_sign = jnp.where(t_place == 0, -1.0, 1.0).astype(jnp.float32)
    high_sign = jnp.where(t_place == t_count - 1, -1.0, 1.0).astype(jnp.float32)

    barrier = pltpu.get_barrier_semaphore()
    for target in (t_next, t_prev, z_next, z_prev):
        pl.semaphore_signal(barrier, inc=1, device_id=target, device_id_type=MESH)

    groups = [(x_hbm, psi_in)]
    for mu in range(4):
        part = pl.ds(18 * mu, 18)
        groups.append((u_hbm.at[part], link_in.at[part]))
    groups.append((c_hbm, clov_in))
    for n in (0, 3, 4, 1, 2, 5):
        for src, dst in parts_of(*groups[n]):
            pltpu.make_async_copy(src, dst, in_sem.at[n]).start()

    def arrived(n):
        held = groups[n][1]
        pltpu.make_async_copy(held, held, in_sem.at[n]).wait()

    def window(v):
        return pl.ds(pl.multiple_of(v * TILE, TILE), TILE)

    def load_spinor(ref, at):
        return [[(ref[3 * s + c, at, :], ref[12 + 3 * s + c, at, :]) for c in range(3)] for s in range(4)]

    def load_half(ref, mu, at):
        return [[(ref[mu, 3 * s + c, at, :], ref[mu, 6 + 3 * s + c, at, :]) for c in range(3)] for s in range(2)]

    def store_half(ref, mu, at, value):
        for s in range(2):
            for c in range(3):
                ref[mu, 3 * s + c, at, :] = value[s][c][0]
                ref[mu, 6 + 3 * s + c, at, :] = value[s][c][1]

    def load_link(mu, at):
        return [[(link[18 * mu + 3 * a + b, at, :], link[18 * mu + 9 + 3 * a + b, at, :]) for b in range(3)] for a in range(3)]

    lane = lax.broadcasted_iota(jnp.int32, (rows, LANES), 1)
    row = lax.broadcasted_iota(jnp.int32, (rows, LANES), 0)
    lane_in = lax.rem(lane, NX)
    row_in = lax.rem(row, face_t)
    upper = lane >= NX

    def shift_x1(value, step):
        if step == 1:
            near, far = pltpu.roll(value, LANES - 1, 1), pltpu.roll(value, NX - 1, 1)
            return jnp.where(lane_in == NX - 1, far, near)
        near, far = pltpu.roll(value, 1, 1), pltpu.roll(value, LANES - NX + 1, 1)
        return jnp.where(lane_in == 0, far, near)

    def shift_x2(value, step):
        turned = pltpu.roll(value, NX, 1)
        if step == 1:
            near = pltpu.roll(turned, rows - nz, 0)
            far = pltpu.roll(turned, face_t - nz, 0)
            moved = jnp.where(row_in >= face_t - nz, far, near)
            return jnp.where(upper, moved, turned)
        near = pltpu.roll(turned, nz, 0)
        far = pltpu.roll(turned, rows - face_t + nz, 0)
        moved = jnp.where(row_in < nz, far, near)
        return jnp.where(upper, turned, moved)

    def z_ahead(src, dst, c):
        for z in range(nz - 1):
            dst[2, c, pl.ds(z, face_z, nz), :] = src[2, c, pl.ds(z + 1, face_z, nz), :]

    def z_behind(src, dst, c):
        for z in range(1, nz):
            dst[2, c, pl.ds(z, face_z, nz), :] = src[2, c, pl.ds(z - 1, face_z, nz), :]

    def t_ahead(src, dst, c):
        dst[3, c, pl.ds(0, rows - face_t), :] = src[3, c, pl.ds(face_t, rows - face_t), :]

    def t_behind(src, dst, c):
        dst[3, c, pl.ds(face_t, rows - face_t), :] = src[3, c, pl.ds(0, rows - face_t), :]

    def for_each(count, body):
        def step(i, carry):
            body(i)
            return carry

        lax.fori_loop(0, count, step, 0)

    targets = (t_prev, t_next, z_prev, z_next, t_prev, z_prev)
    sends = [
        pltpu.make_async_remote_copy(
            src_ref=face_out.at[k], dst_ref=face_in.at[k], send_sem=send_sem.at[k],
            recv_sem=recv_sem.at[k], device_id=targets[k], device_id_type=MESH,
        )
        for k in range(6)
    ]

    def project(mu, v):
        at = window(v)
        field = load_spinor(psi, at)
        store_half(hm, mu, at, half(mu, field, -1.0))
        ahead = half(mu, field, 1.0)
        store_half(hp, mu, at, ahead)
        store_half(bl, mu, at, mat_vec(load_link(mu, at), ahead, True))

    def face(k, c, size):
        return k, pl.ds(c * size, size)

    arrived(0)
    arrived(3)
    for_each(chunks, lambda v: project(2, v))
    for c in range(12):
        k, at = face(3, c, face_z)
        face_out[k, at, :] = bl[2, c, pl.ds(nz - 1, face_z, nz), :]
    pl.semaphore_wait(barrier, 4)
    sends[3].start()
    for c in range(12):
        k, at = face(2, c, face_z)
        face_out[k, at, :] = hm[2, c, pl.ds(0, face_z, nz), :]
    arrived(4)
    for_each(chunks, lambda v: project(3, v))
    for c in range(12):
        k, at = face(0, c, face_t)
        face_out[k, at, :] = hm[3, c, 0:face_t, :]
        k, at = face(1, c, face_t)
        face_out[k, at, :] = bl[3, c, rows - face_t:rows, :]
    sends[1].start()
    sends[0].start()
    sends[2].start()

    arrived(1)
    for_each(chunks, lambda v: project(0, v))
    arrived(2)
    for_each(chunks, lambda v: project(1, v))

    def shifts(c):
        sh_hm[0, c] = shift_x1(hm[0, c], 1)
        sh_bl[0, c] = shift_x1(bl[0, c], -1)
        sh_hm[1, c] = shift_x2(hm[1, c], 1)
        sh_bl[1, c] = shift_x2(bl[1, c], -1)
        z_ahead(hm, sh_hm, c)
        z_behind(bl, sh_bl, c)
        t_ahead(hm, sh_hm, c)
        t_behind(bl, sh_bl, c)

    for_each(12, shifts)

    def hop(mu, at, total):
        ahead = mat_vec(load_link(mu, at), load_half(sh_hm, mu, at), False)
        store_half(prod, mu, at, ahead)
        total = add_whole(mu, total, ahead, -1.0)
        return add_whole(mu, total, load_half(sh_bl, mu, at), 1.0)

    zero = jnp.zeros((TILE, LANES), jnp.float32)

    arrived(5)

    def local(v):
        at = window(v)
        field = load_spinor(psi, at)
        total = [[(zero, zero)] * 3 for _ in range(4)]
        for mu in (0, 1):
            total = hop(mu, at, total)
        for s in range(4):
            for c in range(3):
                base = 36 * (s // 2) + 6 * (3 * (s % 2) + c)
                re = (4.0 + bare_mass) * field[s][c][0] - 0.5 * total[s][c][0]
                im = (4.0 + bare_mass) * field[s][c][1] - 0.5 * total[s][c][1]
                for k in range(6):
                    other = field[2 * (s // 2) + k // 3][k % 3]
                    c_re = clov[base + k, at, :]
                    c_im = clov[72 + base + k, at, :]
                    re = re + (c_re * other[0] - c_im * other[1])
                    im = im + (c_re * other[1] + c_im * other[0])
                acc[3 * s + c, at, :] = re
                acc[12 + 3 * s + c, at, :] = im

    for_each(chunks, local)

    for k in (0, 1, 3):
        sends[k].wait_recv()
    for c in range(12):
        k, at = face(0, c, face_t)
        sh_hm[3, c, pl.ds(rows - face_t, face_t), :] = face_in[k, at, :] * high_sign
        k, at = face(1, c, face_t)
        sh_bl[3, c, pl.ds(0, face_t), :] = face_in[k, at, :] * low_sign
        k, at = face(3, c, face_z)
        sh_bl[2, c, pl.ds(0, face_z, nz), :] = face_in[k, at, :]
        sh_hm[2, c, pl.ds(nz - 1, face_z, nz), :] = jnp.zeros((face_z, LANES), jnp.float32)

    def finish(v, early):
        at = window(v)
        total = [[(zero, zero)] * 3 for _ in range(4)]
        for mu in (2, 3):
            total = hop(mu, at, total)
        held = load_spinor(acc, at)
        phi = [
            [(held[s][c][0] - 0.5 * total[s][c][0], held[s][c][1] - 0.5 * total[s][c][1]) for c in range(3)]
            for s in range(4)
        ]
        if early:
            store_half(hphi, 2, at, half(2, phi, 1.0))
            return
        for s in range(4):
            for c in range(3):
                out_ref[3 * s + c, at, :] = phi[s][c][0]
                out_ref[12 + 3 * s + c, at, :] = phi[s][c][1]
        for mu in range(4):
            store_half(hphi, mu, at, half(mu, phi, 1.0))

    for_each(chunks, lambda v: finish(v, True))
    for c in range(12):
        k, at = face(5, c, face_z)
        face_out[k, at, :] = hphi[2, c, pl.ds(0, face_z, nz), :]
    sends[5].start()

    sends[2].wait_recv()
    for c in range(12):
        k, at = face(2, c, face_z)
        sh_hm[2, c, pl.ds(nz - 1, face_z, nz), :] = face_in[k, at, :]
    for_each(chunks, lambda v: finish(v, False))
    for c in range(12):
        k, at = face(4, c, face_t)
        face_out[k, at, :] = hphi[3, c, 0:face_t, :]
    sends[4].start()

    def shifts_phi(c):
        sh_hphi[0, c] = shift_x1(hphi[0, c], 1)
        sh_hphi[1, c] = shift_x2(hphi[1, c], 1)
        z_ahead(hphi, sh_hphi, c)
        t_ahead(hphi, sh_hphi, c)

    for_each(12, shifts_phi)

    def force(mu, v):
        at = window(v)
        second = mat_vec(load_link(mu, at), load_half(sh_hphi, mu, at), False)
        second_right = load_half(hp, mu, at)
        first = load_half(prod, mu, at)
        first_right = half(mu, load_spinor(out_ref, at), -1.0)
        pairs = [(first[s], first_right[s]) for s in range(2)] + [(second[s], second_right[s]) for s in range(2)]

        def w_re(a, b):
            return csum([l[a][0] * r[b][0] + l[a][1] * r[b][1] for l, r in pairs])

        def w_im(a, b):
            return csum([l[a][1] * r[b][0] - l[a][0] * r[b][1] for l, r in pairs])

        diag = [w_im(a, a) for a in range(3)]
        third = (diag[0] + diag[1] + diag[2]) * (1.0 / 3.0)
        base = 18 * mu
        for a in range(3):
            force_ref[base + 4 * a, at, :] = zero
            force_ref[base + 9 + 4 * a, at, :] = diag[a] - third
            for b in range(a + 1, 3):
                re = 0.5 * (w_re(a, b) - w_re(b, a))
                im = 0.5 * (w_im(a, b) + w_im(b, a))
                force_ref[base + 3 * a + b, at, :] = re
                force_ref[base + 3 * b + a, at, :] = -re
                force_ref[base + 9 + 3 * a + b, at, :] = im
                force_ref[base + 9 + 3 * b + a, at, :] = im

    for mu in (0, 1):
        for_each(chunks, lambda v: force(mu, v))

    sends[4].wait_recv()
    for c in range(12):
        k, at = face(4, c, face_t)
        sh_hphi[3, c, pl.ds(rows - face_t, face_t), :] = face_in[k, at, :] * high_sign
    for_each(chunks, lambda v: force(3, v))
    sends[5].wait_recv()
    for c in range(12):
        k, at = face(5, c, face_z)
        sh_hphi[2, c, pl.ds(nz - 1, face_z, nz), :] = face_in[k, at, :]
    for_each(chunks, lambda v: force(2, v))
    for k in range(6):
        sends[k].wait_send()


def body(spinor, links, clover):
    nt, nz = spinor.shape[3], spinor.shape[4]
    sites = spinor.shape[-3:]
    x, u, c = (a.reshape((-1,) + sites) for a in (spinor, links, clover))
    parts = nt * (sites[2] // LANES)
    rows = parts * nz
    face = max(rows // nt, rows // nz)

    def halves():
        return pltpu.VMEM((4, 12, rows, LANES), jnp.float32)

    def held(array):
        return pltpu.VMEM((array.shape[0], parts, nz, LANES), jnp.float32)

    phi, anti = pl.pallas_call(
        lambda *refs: kernel(nt, nz, *refs),
        name="wilson",
        out_shape=(
            pltpu.VMEM((24, parts, nz, LANES), jnp.float32),
            pltpu.VMEM((u.shape[0], parts, nz, LANES), jnp.float32),
        ),
        in_specs=[pl.BlockSpec(memory_space=pltpu.HBM)] * 3,
        out_specs=(pl.BlockSpec(memory_space=pltpu.VMEM),) * 2,
        scratch_shapes=[
            held(x), held(u), held(c),
            halves(), halves(), halves(), halves(), halves(), halves(),
            pltpu.VMEM((24, rows, LANES), jnp.float32),
            halves(), halves(),
            pltpu.VMEM((6, 12 * face, LANES), jnp.float32),
            pltpu.VMEM((6, 12 * face, LANES), jnp.float32),
            pltpu.SemaphoreType.DMA((6,)),
            pltpu.SemaphoreType.DMA((6,)),
            pltpu.SemaphoreType.DMA((6,)),
        ],
        compiler_params=pltpu.CompilerParams(collective_id=0, has_side_effects=True, vmem_limit_bytes=56 * 1024 * 1024),
    )(x, u, c)
    applied, force = pl.pallas_call(
        write_out,
        name="write_out",
        out_shape=(
            jax.ShapeDtypeStruct(x.shape, jnp.float32),
            jax.ShapeDtypeStruct(u.shape, jnp.float32),
        ),
        in_specs=[pl.BlockSpec(memory_space=pltpu.VMEM)] * 2,
        out_specs=(pl.BlockSpec(memory_space=pl.ANY),) * 2,
        scratch_shapes=[pltpu.SemaphoreType.DMA((2,))],
        compiler_params=pltpu.CompilerParams(vmem_limit_bytes=8 * 1024 * 1024),
    )(phi, anti)
    return applied.reshape(spinor.shape), force.reshape(links.shape)


def solution(mesh):
    return jax.shard_map(
        body,
        mesh=mesh,
        in_specs=(
            P(None, None, None, "ta", "gz", None),
            P(None, None, None, None, "ta", "gz", None),
            P(None, None, None, None, "ta", "gz", None),
        ),
        out_specs=(
            P(None, None, None, "ta", "gz", None),
            P(None, None, None, None, "ta", "gz", None),
        ),
        check_vma=False,
    )
```

```python
import jax
import jax.numpy as jnp
from jax import lax
from jax.experimental import pallas as pl
from jax.experimental.pallas import tpu as pltpu
from jax.sharding import PartitionSpec as P

NX = 64
LANES = 128
TILE = 8
MESH = pl.DeviceIdType.MESH

bare_mass = -0.25
gamma_table = (
    ((3, 0.0, -1.0), (2, 0.0, -1.0), (1, 0.0, 1.0), (0, 0.0, 1.0)),
    ((3, -1.0, 0.0), (2, 1.0, 0.0), (1, 1.0, 0.0), (0, -1.0, 0.0)),
    ((2, 0.0, -1.0), (3, 0.0, 1.0), (0, 0.0, 1.0), (1, 0.0, -1.0)),
    ((2, 1.0, 0.0), (3, 1.0, 0.0), (0, 1.0, 0.0), (1, 1.0, 0.0)),
)


def add_signed(a, b, positive):
    return a + b if positive else a - b


def add_phase(a, b, phase_re, phase_im):
    if phase_im == 0.0:
        up = phase_re > 0
        return (add_signed(a[0], b[0], up), add_signed(a[1], b[1], up))
    up = phase_im > 0
    return (add_signed(a[0], b[1], not up), add_signed(a[1], b[0], up))


def half(mu, field, sign):
    out = []
    for s in range(2):
        source, p_re, p_im = gamma_table[mu][s]
        out.append(
            [add_phase(field[s][c], field[source][c], sign * p_re, sign * p_im) for c in range(3)]
        )
    return out


def add_whole(mu, total, halves, sign):
    out = [[add_phase(total[s][c], halves[s][c], 1.0, 0.0) for c in range(3)] for s in range(2)]
    for s in (2, 3):
        source, p_re, p_im = gamma_table[mu][s]
        out.append(
            [add_phase(total[s][c], halves[source][c], sign * p_re, sign * p_im) for c in range(3)]
        )
    return out


def csum(terms):
    total = terms[0]
    for term in terms[1:]:
        total = total + term
    return total


def mat_vec(link, vec, dagger):
    out = []
    for s in range(2):
        rows = []
        for a in range(3):
            re, im = [], []
            for b in range(3):
                h = vec[s][b]
                if dagger:
                    m = link[b][a]
                    re.append(m[0] * h[0] + m[1] * h[1])
                    im.append(m[0] * h[1] - m[1] * h[0])
                else:
                    m = link[a][b]
                    re.append(m[0] * h[0] - m[1] * h[1])
                    im.append(m[0] * h[1] + m[1] * h[0])
            rows.append((csum(re), csum(im)))
        out.append(rows)
    return out


def flat(ref):
    return ref.reshape(ref.shape[0], ref.shape[1] * ref.shape[2], ref.shape[3])


def parts_of(whole, held):
    parts = whole.shape[-1] // LANES
    for t in range(whole.shape[-3]):
        for q in range(parts):
            yield whole.at[:, t, :, pl.ds(LANES * q, LANES)], held.at[:, parts * t + q]


def write_out(phi_ref, force_ref, out_hbm, force_hbm, sem):
    for n, (whole, held) in enumerate(((force_hbm, force_ref), (out_hbm, phi_ref))):
        for dst, src in parts_of(whole, held):
            pltpu.make_async_copy(src, dst, sem.at[n]).start()
    for n, held in enumerate((force_ref, phi_ref)):
        pltpu.make_async_copy(held, held, sem.at[n]).wait()


def kernel(nt, nz, x_hbm, u_hbm, c_hbm, phi_out, force_out, psi_in, link_in, clov_in, hm, hp, bl,
           sh_hm, sh_bl, prod, acc, hphi, sh_hphi, face_out, face_in, in_sem, send_sem, recv_sem, ready):
    psi, link, clov, out_ref, force_ref = map(flat, (psi_in, link_in, clov_in, phi_out, force_out))
    rows = psi.shape[1]
    face_t = rows // nt
    face_z = rows // nz
    line = face_t // nz
    chunks = rows // TILE
    t_place, z_place = lax.axis_index("ta"), lax.axis_index("gz")
    t_count, z_count = lax.axis_size("ta"), lax.axis_size("gz")
    low_sign = jnp.where(t_place == 0, -1.0, 1.0).astype(jnp.float32)
    high_sign = jnp.where(t_place == t_count - 1, -1.0, 1.0).astype(jnp.float32)

    near = (
        (lax.rem(t_place + t_count - 1, t_count), z_place),
        (lax.rem(t_place + 1, t_count), z_place),
        (t_place, lax.rem(z_place + z_count - 1, z_count)),
        (t_place, lax.rem(z_place + 1, z_count)),
    )
    T_PREV, T_NEXT, Z_PREV, Z_NEXT = range(4)
    first = (t_place > 0, t_place == t_count - 1, z_place > 0, z_place == z_count - 1)
    barrier = pltpu.get_barrier_semaphore()

    groups = [(x_hbm, psi_in)]
    for mu in range(4):
        part = pl.ds(18 * mu, 18)
        groups.append((u_hbm.at[part], link_in.at[part]))
    groups.append((c_hbm, clov_in))

    def fetch(n):
        for src, dst in parts_of(*groups[n]):
            pltpu.make_async_copy(src, dst, in_sem.at[n]).start()

    def arrived(n):
        held = groups[n][1]
        pltpu.make_async_copy(held, held, in_sem.at[n]).wait()

    for k in range(4):
        @pl.when(jnp.logical_not(first[k]))
        def _():
            pl.semaphore_signal(barrier, inc=1, device_id=near[k], device_id_type=MESH)

    for n in (0, 3, 4):
        fetch(n)
    greeters = sum(f.astype(jnp.int32) for f in first)

    @pl.when(greeters > 0)
    def _():
        pl.semaphore_wait(barrier, greeters)

    for k in range(4):
        @pl.when(first[k])
        def _():
            pl.semaphore_signal(ready.at[k ^ 1], inc=1, device_id=near[k], device_id_type=MESH)
    for n in (1, 2, 5):
        fetch(n)

    def window(v):
        return pl.ds(pl.multiple_of(v * TILE, TILE), TILE)

    def load_spinor(ref, at):
        return [[(ref[3 * s + c, at, :], ref[12 + 3 * s + c, at, :]) for c in range(3)] for s in range(4)]

    def store_spinor(ref, at, value):
        for s in range(4):
            for c in range(3):
                ref[3 * s + c, at, :] = value[s][c][0]
                ref[12 + 3 * s + c, at, :] = value[s][c][1]

    def load_half(ref, mu, at):
        return [[(ref[mu, 3 * s + c, at, :], ref[mu, 6 + 3 * s + c, at, :]) for c in range(3)] for s in range(2)]

    def store_half(ref, mu, at, value):
        for s in range(2):
            for c in range(3):
                ref[mu, 3 * s + c, at, :] = value[s][c][0]
                ref[mu, 6 + 3 * s + c, at, :] = value[s][c][1]

    def load_link(mu, at):
        return [[(link[18 * mu + 3 * a + b, at, :], link[18 * mu + 9 + 3 * a + b, at, :]) for b in range(3)] for a in range(3)]

    lane = lax.broadcasted_iota(jnp.int32, (rows, LANES), 1)
    row = lax.broadcasted_iota(jnp.int32, (rows, LANES), 0)
    lane_in = lax.rem(lane, NX)
    row_in = lax.rem(row, face_t)
    upper = lane >= NX

    def shift_x1(value, step):
        if step == 1:
            near, far = pltpu.roll(value, LANES - 1, 1), pltpu.roll(value, NX - 1, 1)
            return jnp.where(lane_in == NX - 1, far, near)
        near, far = pltpu.roll(value, 1, 1), pltpu.roll(value, LANES - NX + 1, 1)
        return jnp.where(lane_in == 0, far, near)

    def shift_x2(value, step):
        turned = pltpu.roll(value, NX, 1)
        if step == 1:
            near = pltpu.roll(turned, rows - nz, 0)
            far = pltpu.roll(turned, face_t - nz, 0)
            moved = jnp.where(row_in >= face_t - nz, far, near)
            return jnp.where(upper, moved, turned)
        near = pltpu.roll(turned, nz, 0)
        far = pltpu.roll(turned, rows - face_t + nz, 0)
        moved = jnp.where(row_in < nz, far, near)
        return jnp.where(upper, turned, moved)

    def z_ahead(src, dst, c):
        for z in range(nz - 1):
            dst[2, c, pl.ds(z, face_z, nz), :] = src[2, c, pl.ds(z + 1, face_z, nz), :]

    def z_behind(src, dst, c):
        for z in range(1, nz):
            dst[2, c, pl.ds(z, face_z, nz), :] = src[2, c, pl.ds(z - 1, face_z, nz), :]

    def t_ahead(src, dst, c):
        dst[3, c, pl.ds(0, rows - face_t), :] = src[3, c, pl.ds(face_t, rows - face_t), :]

    def t_behind(src, dst, c):
        dst[3, c, pl.ds(face_t, rows - face_t), :] = src[3, c, pl.ds(0, rows - face_t), :]

    def for_each(count, body, low=0):
        def step(i, carry):
            body(i)
            return carry

        lax.fori_loop(low, count, step, 0)

    t_last, z_last = nt - 1, nz - 1
    messages = {
        "a0": (T_PREV, [(0, 0)], [(t_last, 0)]),
        "a1": (T_PREV, [(0, z) for z in range(1, nz)], [(t_last, z) for z in range(1, nz)]),
        "b0": (T_NEXT, [(t_last, 0)], [(0, 0)]),
        "b1": (T_NEXT, [(t_last, z) for z in range(1, nz)], [(0, z) for z in range(1, nz)]),
        "c0": (Z_PREV, [(0, 0)], [(0, z_last)]),
        "c1": (Z_PREV, [(t, 0) for t in range(1, nt)], [(t, z_last) for t in range(1, nt)]),
        "d0": (Z_NEXT, [(0, z_last)], [(0, 0)]),
        "d1": (Z_NEXT, [(t, z_last) for t in range(1, nt)], [(t, 0) for t in range(1, nt)]),
        "e0": (Z_PREV, [(t, 0) for t in range(t_last)], [(t, z_last) for t in range(t_last)]),
        "e1": (Z_PREV, [(t_last, 0)], [(t_last, z_last)]),
        "f0": (T_PREV, [(0, z) for z in range(z_last)], [(t_last, z) for z in range(z_last)]),
        "f1": (T_PREV, [(0, z_last)], [(t_last, z_last)]),
    }
    names = list(messages)

    def place(name, i, c):
        return names.index(name), pl.ds((12 * i + c) * line, line)

    def lines(at):
        return pl.ds(at[0] * face_t + at[1], line, nz)

    def pack(name, src, mu):
        for i, at in enumerate(messages[name][1]):
            for c in range(12):
                k, held = place(name, i, c)
                face_out[k, held, :] = src[mu, c, lines(at), :]

    def unpack(name, dst, mu, change=lambda value, at, c: value):
        for i, at in enumerate(messages[name][2]):
            for c in range(12):
                k, held = place(name, i, c)
                dst[mu, c, lines(at), :] = change(face_in[k, held, :], at, c)

    def copy_of(name):
        k, size = names.index(name), 12 * line * len(messages[name][1])
        return pltpu.make_async_remote_copy(
            src_ref=face_out.at[k, pl.ds(0, size)], dst_ref=face_in.at[k, pl.ds(0, size)], send_sem=send_sem.at[k],
            recv_sem=recv_sem.at[k], device_id=near[messages[name][0]], device_id_type=MESH,
        )

    copies = {name: copy_of(name) for name in names}
    greeted = set()

    def send_early(*some):
        for name in some:
            pl.when(first[messages[name][0]])(copies[name].start)

    def send_late(*some):
        for name in some:
            side = messages[name][0]

            @pl.when(jnp.logical_not(first[side]))
            def _():
                if side not in greeted:
                    pl.semaphore_wait(ready.at[side], 1)
                copies[name].start()

            greeted.add(side)

    def received(*some):
        for name in some:
            copies[name].wait_recv()

    def project(mu, v):
        at = window(v)
        field = load_spinor(psi, at)
        store_half(hm, mu, at, half(mu, field, -1.0))
        ahead = half(mu, field, 1.0)
        store_half(hp, mu, at, ahead)
        store_half(bl, mu, at, mat_vec(load_link(mu, at), ahead, True))

    arrived(0)
    arrived(3)
    for_each(chunks, lambda v: project(2, v))
    for name in ("d0", "d1"):
        pack(name, bl, 2)
    for name in ("c0", "c1"):
        pack(name, hm, 2)
    send_early("d0")
    arrived(4)
    for_each(chunks, lambda v: project(3, v))
    for name in ("a0", "a1"):
        pack(name, hm, 3)
    for name in ("b0", "b1"):
        pack(name, bl, 3)
    send_early("b0", "a0", "c0")
    send_late("b0", "d0")
    send_early("d1", "b1", "a1", "c1")
    send_late("b1", "d1")

    arrived(1)
    for_each(chunks, lambda v: project(0, v))
    arrived(2)
    for_each(chunks, lambda v: project(1, v))

    for c in range(12):
        sh_hm[0, c] = shift_x1(hm[0, c], 1)
        sh_bl[0, c] = shift_x1(bl[0, c], -1)
        sh_hm[1, c] = shift_x2(hm[1, c], 1)
        sh_bl[1, c] = shift_x2(bl[1, c], -1)
        z_ahead(hm, sh_hm, c)
        z_behind(bl, sh_bl, c)
        t_ahead(hm, sh_hm, c)
        t_behind(bl, sh_bl, c)

    def hop(mu, at, total):
        ahead = mat_vec(load_link(mu, at), load_half(sh_hm, mu, at), False)
        store_half(prod, mu, at, ahead)
        total = add_whole(mu, total, ahead, -1.0)
        return add_whole(mu, total, load_half(sh_bl, mu, at), 1.0)

    zero = jnp.zeros((TILE, LANES), jnp.float32)

    def nothing():
        return [[(zero, zero)] * 3 for _ in range(4)]

    arrived(5)

    def local(v):
        at = window(v)
        field = load_spinor(psi, at)
        total = nothing()
        for mu in (0, 1):
            total = hop(mu, at, total)
        for s in range(4):
            for c in range(3):
                base = 36 * (s // 2) + 6 * (3 * (s % 2) + c)
                re = (4.0 + bare_mass) * field[s][c][0] - 0.5 * total[s][c][0]
                im = (4.0 + bare_mass) * field[s][c][1] - 0.5 * total[s][c][1]
                for k in range(6):
                    other = field[2 * (s // 2) + k // 3][k % 3]
                    c_re = clov[base + k, at, :]
                    c_im = clov[72 + base + k, at, :]
                    re = re + (c_re * other[0] - c_im * other[1])
                    im = im + (c_re * other[1] + c_im * other[0])
                acc[3 * s + c, at, :] = re
                acc[12 + 3 * s + c, at, :] = im

    for_each(chunks, local)

    def with_hops(mu, at):
        total = hop(mu, at, nothing())
        held = load_spinor(acc, at)
        return [
            [(held[s][c][0] - 0.5 * total[s][c][0], held[s][c][1] - 0.5 * total[s][c][1]) for c in range(3)]
            for s in range(4)
        ]

    def partial(across, along, v):
        at = window(v)
        store_half(hphi, along, at, half(along, with_hops(across, at), 1.0))

    def signed(sign):
        return lambda value, at, c: value * sign

    low_chunks = -(-face_t // TILE)
    high_chunk = (rows - face_t) // TILE

    send_late("a0", "c0", "a1", "c1")

    received("a0")
    unpack("a0", sh_hm, 3, signed(high_sign))
    for_each(chunks, lambda v: partial(3, 2, v), high_chunk)
    pack("e1", hphi, 2)
    copies["e1"].start()
    received("b0")
    unpack("b0", sh_bl, 3, signed(low_sign))
    for_each(-(-(rows - face_t) // TILE), lambda v: partial(3, 2, v))
    pack("e0", hphi, 2)
    copies["e0"].start()

    received("c0")
    unpack("c0", sh_hm, 2)
    for_each(low_chunks, lambda v: partial(2, 3, v))
    pack("f1", hphi, 3)
    copies["f1"].start()
    received("d0")
    unpack("d0", sh_bl, 2)
    for_each(low_chunks, lambda v: partial(2, 3, v))
    pack("f0", hphi, 3)
    copies["f0"].start()

    received("a1", "b1")
    unpack("a1", sh_hm, 3, signed(high_sign))
    unpack("b1", sh_bl, 3, signed(low_sign))

    def gather(v):
        at = window(v)
        store_spinor(acc, at, with_hops(3, at))

    for_each(chunks, gather)
    received("c1", "d1")
    unpack("c1", sh_hm, 2)
    unpack("d1", sh_bl, 2)

    def finish(v):
        at = window(v)
        phi = with_hops(2, at)
        store_spinor(out_ref, at, phi)
        for mu in range(4):
            store_half(hphi, mu, at, half(mu, phi, 1.0))

    for_each(chunks, finish)

    for c in range(12):
        sh_hphi[0, c] = shift_x1(hphi[0, c], 1)
        sh_hphi[1, c] = shift_x2(hphi[1, c], 1)
        z_ahead(hphi, sh_hphi, c)
        t_ahead(hphi, sh_hphi, c)

    def force(mu, v):
        at = window(v)
        second = mat_vec(load_link(mu, at), load_half(sh_hphi, mu, at), False)
        second_right = load_half(hp, mu, at)
        first = load_half(prod, mu, at)
        first_right = half(mu, load_spinor(out_ref, at), -1.0)
        pairs = [(first[s], first_right[s]) for s in range(2)] + [(second[s], second_right[s]) for s in range(2)]

        def w_re(a, b):
            return csum([l[a][0] * r[b][0] + l[a][1] * r[b][1] for l, r in pairs])

        def w_im(a, b):
            return csum([l[a][1] * r[b][0] - l[a][0] * r[b][1] for l, r in pairs])

        diag = [w_im(a, a) for a in range(3)]
        third = (diag[0] + diag[1] + diag[2]) * (1.0 / 3.0)
        base = 18 * mu
        for a in range(3):
            force_ref[base + 4 * a, at, :] = zero
            force_ref[base + 9 + 4 * a, at, :] = diag[a] - third
            for b in range(a + 1, 3):
                re = 0.5 * (w_re(a, b) - w_re(b, a))
                im = 0.5 * (w_im(a, b) + w_im(b, a))
                force_ref[base + 3 * a + b, at, :] = re
                force_ref[base + 3 * b + a, at, :] = -re
                force_ref[base + 9 + 3 * a + b, at, :] = im
                force_ref[base + 9 + 3 * b + a, at, :] = im

    for mu in (0, 1):
        for_each(chunks, lambda v: force(mu, v))

    for name in ("f0", "f1"):
        received(name)
        unpack(name, sh_hphi, 3, lambda value, at, c: value * high_sign - bl[3, c, lines(at), :])
    for_each(chunks, lambda v: force(3, v))
    for name in ("e0", "e1"):
        received(name)
        unpack(name, sh_hphi, 2, lambda value, at, c: value - bl[2, c, lines(at), :])
    for_each(chunks, lambda v: force(2, v))
    for name in names:
        copies[name].wait_send()


def body(spinor, links, clover):
    nt, nz = spinor.shape[3], spinor.shape[4]
    sites = spinor.shape[-3:]
    x, u, c = (a.reshape((-1,) + sites) for a in (spinor, links, clover))
    parts = nt * (sites[2] // LANES)
    rows = parts * nz
    assert nt > 1 and nz > 1
    face = max(nt - 1, nz - 1) * rows // (nt * nz)

    def halves():
        return pltpu.VMEM((4, 12, rows, LANES), jnp.float32)

    def held(array):
        return pltpu.VMEM((array.shape[0], parts, nz, LANES), jnp.float32)

    phi, anti = pl.pallas_call(
        lambda *refs: kernel(nt, nz, *refs),
        name="wilson",
        out_shape=(
            pltpu.VMEM((24, parts, nz, LANES), jnp.float32),
            pltpu.VMEM((u.shape[0], parts, nz, LANES), jnp.float32),
        ),
        in_specs=[pl.BlockSpec(memory_space=pltpu.HBM)] * 3,
        out_specs=(pl.BlockSpec(memory_space=pltpu.VMEM),) * 2,
        scratch_shapes=[
            held(x), held(u), held(c),
            halves(), halves(), halves(), halves(), halves(), halves(),
            pltpu.VMEM((24, rows, LANES), jnp.float32),
            halves(), halves(),
            pltpu.VMEM((12, 12 * face, LANES), jnp.float32),
            pltpu.VMEM((12, 12 * face, LANES), jnp.float32),
            pltpu.SemaphoreType.DMA((6,)),
            pltpu.SemaphoreType.DMA((12,)),
            pltpu.SemaphoreType.DMA((12,)),
            pltpu.SemaphoreType.REGULAR((4,)),
        ],
        compiler_params=pltpu.CompilerParams(collective_id=0, has_side_effects=True, vmem_limit_bytes=56 * 1024 * 1024),
    )(x, u, c)
    applied, force = pl.pallas_call(
        write_out,
        name="write_out",
        out_shape=(
            jax.ShapeDtypeStruct(x.shape, jnp.float32),
            jax.ShapeDtypeStruct(u.shape, jnp.float32),
        ),
        in_specs=[pl.BlockSpec(memory_space=pltpu.VMEM)] * 2,
        out_specs=(pl.BlockSpec(memory_space=pl.ANY),) * 2,
        scratch_shapes=[pltpu.SemaphoreType.DMA((2,))],
        compiler_params=pltpu.CompilerParams(vmem_limit_bytes=8 * 1024 * 1024),
    )(phi, anti)
    return applied.reshape(spinor.shape), force.reshape(links.shape)


def solution(mesh):
    return jax.shard_map(
        body,
        mesh=mesh,
        in_specs=(
            P(None, None, None, "ta", "gz", None),
            P(None, None, None, None, "ta", "gz", None),
            P(None, None, None, None, "ta", "gz", None),
        ),
        out_specs=(
            P(None, None, None, "ta", "gz", None),
            P(None, None, None, None, "ta", "gz", None),
        ),
        check_vma=False,
    )
```

```python
import jax
import jax.numpy as jnp
from jax import lax
from jax.experimental import pallas as pl
from jax.experimental.pallas import tpu as pltpu
from jax.sharding import PartitionSpec as P

NX = 64
LANES = 128
TILE = 8
MESH = pl.DeviceIdType.MESH

bare_mass = -0.25
gamma_table = (
    ((3, 0.0, -1.0), (2, 0.0, -1.0), (1, 0.0, 1.0), (0, 0.0, 1.0)),
    ((3, -1.0, 0.0), (2, 1.0, 0.0), (1, 1.0, 0.0), (0, -1.0, 0.0)),
    ((2, 0.0, -1.0), (3, 0.0, 1.0), (0, 0.0, 1.0), (1, 0.0, -1.0)),
    ((2, 1.0, 0.0), (3, 1.0, 0.0), (0, 1.0, 0.0), (1, 1.0, 0.0)),
)


def add_signed(a, b, positive):
    return a + b if positive else a - b


def add_phase(a, b, phase_re, phase_im):
    if phase_im == 0.0:
        up = phase_re > 0
        return (add_signed(a[0], b[0], up), add_signed(a[1], b[1], up))
    up = phase_im > 0
    return (add_signed(a[0], b[1], not up), add_signed(a[1], b[0], up))


def half(mu, field, sign):
    out = []
    for s in range(2):
        source, p_re, p_im = gamma_table[mu][s]
        out.append(
            [add_phase(field[s][c], field[source][c], sign * p_re, sign * p_im) for c in range(3)]
        )
    return out


def add_whole(mu, total, halves, sign):
    out = [[add_phase(total[s][c], halves[s][c], 1.0, 0.0) for c in range(3)] for s in range(2)]
    for s in (2, 3):
        source, p_re, p_im = gamma_table[mu][s]
        out.append(
            [add_phase(total[s][c], halves[source][c], sign * p_re, sign * p_im) for c in range(3)]
        )
    return out


def csum(terms):
    total = terms[0]
    for term in terms[1:]:
        total = total + term
    return total


def mat_vec(link, vec, dagger):
    out = []
    for s in range(2):
        rows = []
        for a in range(3):
            re, im = [], []
            for b in range(3):
                h = vec[s][b]
                if dagger:
                    m = link[b][a]
                    re.append(m[0] * h[0] + m[1] * h[1])
                    im.append(m[0] * h[1] - m[1] * h[0])
                else:
                    m = link[a][b]
                    re.append(m[0] * h[0] - m[1] * h[1])
                    im.append(m[0] * h[1] + m[1] * h[0])
            rows.append((csum(re), csum(im)))
        out.append(rows)
    return out


def flat(ref):
    return ref.reshape(ref.shape[0], ref.shape[1] * ref.shape[2], ref.shape[3])


def parts_of(whole, held):
    parts = whole.shape[-1] // LANES
    for t in range(whole.shape[-3]):
        for q in range(parts):
            yield whole.at[:, t, :, pl.ds(LANES * q, LANES)], held.at[:, parts * t + q]


def write_out(phi_ref, force_ref, out_hbm, force_hbm, sem):
    for n, (whole, held) in enumerate(((force_hbm, force_ref), (out_hbm, phi_ref))):
        for dst, src in parts_of(whole, held):
            pltpu.make_async_copy(src, dst, sem.at[n]).start()
    for n, held in enumerate((force_ref, phi_ref)):
        pltpu.make_async_copy(held, held, sem.at[n]).wait()


def kernel(nt, nz, x_hbm, u_hbm, c_hbm, phi_out, force_out, psi_in, link_in, clov_in, hm, hp, bl,
           sh_hm, sh_bl, prod, acc, hphi, sh_hphi, face_out, face_in, link_out, corner_in, in_sem,
           send_sem, recv_sem, ready):
    psi, link, clov, out_ref, force_ref = map(flat, (psi_in, link_in, clov_in, phi_out, force_out))
    rows = psi.shape[1]
    face_t = rows // nt
    face_z = rows // nz
    line = face_t // nz
    chunks = rows // TILE
    t_place, z_place = lax.axis_index("ta"), lax.axis_index("gz")
    t_count, z_count = lax.axis_size("ta"), lax.axis_size("gz")
    low_sign = jnp.where(t_place == 0, -1.0, 1.0).astype(jnp.float32)
    high_sign = jnp.where(t_place == t_count - 1, -1.0, 1.0).astype(jnp.float32)

    T_PREV, T_NEXT, Z_PREV, Z_NEXT = range(4)
    near = (
        (lax.rem(t_place + t_count - 1, t_count), z_place),
        (lax.rem(t_place + 1, t_count), z_place),
        (t_place, lax.rem(z_place + z_count - 1, z_count)),
        (t_place, lax.rem(z_place + 1, z_count)),
    )
    first = (t_place > 0, t_place == t_count - 1, z_place > 0, z_place == z_count - 1)
    barrier = pltpu.get_barrier_semaphore()

    groups = [(x_hbm, psi_in)]
    for mu in range(4):
        part = pl.ds(18 * mu, 18)
        groups.append((u_hbm.at[part], link_in.at[part]))
    groups.append((c_hbm, clov_in))

    def fetch(n):
        for src, dst in parts_of(*groups[n]):
            pltpu.make_async_copy(src, dst, in_sem.at[n]).start()

    def arrived(n):
        held = groups[n][1]
        pltpu.make_async_copy(held, held, in_sem.at[n]).wait()

    even = lax.rem(t_place, 2) == 0
    relay = jnp.logical_and(even, t_place > 0)
    t_after = near[T_NEXT][0]
    relayed = jnp.logical_and(lax.rem(t_after, 2) == 0, t_after > 0)
    z_low, z_high = z_place == 0, z_place == z_count - 1

    def greet(k, when):
        @pl.when(jnp.logical_and(when, jnp.logical_not(first[k])))
        def _():
            pl.semaphore_signal(barrier, inc=1, device_id=near[k], device_id_type=MESH)

    for k in range(4):
        greet(k, jnp.logical_not(relay) if k == Z_PREV else True)

    for n in (0, 3, 4):
        fetch(n)
    greeters = sum(f.astype(jnp.int32) for f in first)

    @pl.when(greeters > 0)
    def _():
        pl.semaphore_wait(barrier, greeters)

    greet(Z_PREV, relay)
    for k in range(4):
        @pl.when(first[k])
        def _():
            pl.semaphore_signal(ready.at[k ^ 1], inc=1, device_id=near[k], device_id_type=MESH)
    for n in (1, 2, 5):
        fetch(n)

    def window(v):
        return pl.ds(pl.multiple_of(v * TILE, TILE), TILE)

    def load_spinor(ref, at):
        return [[(ref[3 * s + c, at, :], ref[12 + 3 * s + c, at, :]) for c in range(3)] for s in range(4)]

    def store_spinor(ref, at, value):
        for s in range(4):
            for c in range(3):
                ref[3 * s + c, at, :] = value[s][c][0]
                ref[12 + 3 * s + c, at, :] = value[s][c][1]

    def load_half(ref, mu, at):
        return [[(ref[mu, 3 * s + c, at, :], ref[mu, 6 + 3 * s + c, at, :]) for c in range(3)] for s in range(2)]

    def store_half(ref, mu, at, value):
        for s in range(2):
            for c in range(3):
                ref[mu, 3 * s + c, at, :] = value[s][c][0]
                ref[mu, 6 + 3 * s + c, at, :] = value[s][c][1]

    def load_link(mu, at):
        return [[(link[18 * mu + 3 * a + b, at, :], link[18 * mu + 9 + 3 * a + b, at, :]) for b in range(3)] for a in range(3)]

    lane = lax.broadcasted_iota(jnp.int32, (rows, LANES), 1)
    row = lax.broadcasted_iota(jnp.int32, (rows, LANES), 0)
    lane_in = lax.rem(lane, NX)
    row_in = lax.rem(row, face_t)
    upper = lane >= NX

    def shift_x1(value, step):
        if step == 1:
            near, far = pltpu.roll(value, LANES - 1, 1), pltpu.roll(value, NX - 1, 1)
            return jnp.where(lane_in == NX - 1, far, near)
        near, far = pltpu.roll(value, 1, 1), pltpu.roll(value, LANES - NX + 1, 1)
        return jnp.where(lane_in == 0, far, near)

    def shift_x2(value, step):
        turned = pltpu.roll(value, NX, 1)
        if step == 1:
            near = pltpu.roll(turned, rows - nz, 0)
            far = pltpu.roll(turned, face_t - nz, 0)
            moved = jnp.where(row_in >= face_t - nz, far, near)
            return jnp.where(upper, moved, turned)
        near = pltpu.roll(turned, nz, 0)
        far = pltpu.roll(turned, rows - face_t + nz, 0)
        moved = jnp.where(row_in < nz, far, near)
        return jnp.where(upper, turned, moved)

    def z_ahead(src, dst, c):
        for z in range(nz - 1):
            dst[2, c, pl.ds(z, face_z, nz), :] = src[2, c, pl.ds(z + 1, face_z, nz), :]

    def z_behind(src, dst, c):
        for z in range(1, nz):
            dst[2, c, pl.ds(z, face_z, nz), :] = src[2, c, pl.ds(z - 1, face_z, nz), :]

    def t_ahead(src, dst, c):
        dst[3, c, pl.ds(0, rows - face_t), :] = src[3, c, pl.ds(face_t, rows - face_t), :]

    def t_behind(src, dst, c):
        dst[3, c, pl.ds(face_t, rows - face_t), :] = src[3, c, pl.ds(0, rows - face_t), :]

    def for_each(count, body, low=0):
        def step(i, carry):
            body(i)
            return carry

        lax.fori_loop(low, count, step, 0)

    t_last, z_last = nt - 1, nz - 1
    messages = {
        "a0": (T_PREV, [(0, 0)], [(t_last, 0)]),
        "a1": (T_PREV, [(0, z) for z in range(1, nz)], [(t_last, z) for z in range(1, nz)]),
        "b0": (T_NEXT, [(t_last, 0)], [(0, 0)]),
        "b1": (T_NEXT, [(t_last, z) for z in range(1, nz)], [(0, z) for z in range(1, nz)]),
        "c0": (Z_PREV, [(0, 0)], [(0, z_last)]),
        "c1": (Z_PREV, [(t, 0) for t in range(1, nt)], [(t, z_last) for t in range(1, nt)]),
        "d0": (Z_NEXT, [(0, z_last)], [(0, 0)]),
        "d1": (Z_NEXT, [(t, z_last) for t in range(1, nt)], [(t, 0) for t in range(1, nt)]),
        "e0": (Z_PREV, [(t, 0) for t in range(t_last)], [(t, z_last) for t in range(t_last)]),
        "e1": (Z_PREV, [(t_last, 0)], [(t_last, z_last)]),
        "f0": (T_PREV, [(0, z) for z in range(z_last)], [(t_last, z) for z in range(z_last)]),
        "f1": (T_PREV, [(0, z_last)], [(t_last, z_last)]),
    }
    names = list(messages)

    def place(name, i, c):
        return names.index(name), pl.ds((12 * i + c) * line, line)

    def lines(at):
        return pl.ds(at[0] * face_t + at[1], line, nz)

    def pack(name, src, mu):
        for i, at in enumerate(messages[name][1]):
            for c in range(12):
                k, held = place(name, i, c)
                face_out[k, held, :] = src[mu, c, lines(at), :]

    def unpack(name, dst, mu, change=lambda value, at, c: value):
        for i, at in enumerate(messages[name][2]):
            for c in range(12):
                k, held = place(name, i, c)
                dst[mu, c, lines(at), :] = change(face_in[k, held, :], at, c)

    def copy_of(name):
        k, size = names.index(name), 12 * line * len(messages[name][1])
        return pltpu.make_async_remote_copy(
            src_ref=face_out.at[k, pl.ds(0, size)], dst_ref=face_in.at[k, pl.ds(0, size)], send_sem=send_sem.at[k],
            recv_sem=recv_sem.at[k], device_id=near[messages[name][0]], device_id_type=MESH,
        )

    copies = {name: copy_of(name) for name in names}

    def corner_of(k, held, target):
        size = pl.ds(0, held.shape[0])
        return pltpu.make_async_remote_copy(
            src_ref=held, dst_ref=corner_in.at[k, size], send_sem=send_sem.at[len(names) + k],
            recv_sem=recv_sem.at[len(names) + k], device_id=target, device_id_type=MESH,
        )

    t_before = near[T_PREV][0]
    corners = [
        corner_of(0, face_out.at[names.index("d0"), pl.ds(0, 12 * line)], (t_before, near[Z_NEXT][1])),
        corner_of(1, face_out.at[names.index("c0"), pl.ds(0, 12 * line)], (t_before, near[Z_PREV][1])),
        corner_of(2, link_out, near[T_PREV]),
    ]
    relay_high, relay_low = jnp.logical_and(relay, z_high), jnp.logical_and(relay, z_low)
    relayed_high, relayed_low = jnp.logical_and(relayed, z_high), jnp.logical_and(relayed, z_low)
    def sender(mine):
        greeted = set()

        def early(*some):
            for name in some:
                pl.when(jnp.logical_and(mine, first[messages[name][0]]))(copies[name].start)

        def late(*some):
            for name in some:
                side = messages[name][0]

                @pl.when(jnp.logical_and(mine, jnp.logical_not(first[side])))
                def _():
                    if side not in greeted:
                        pl.semaphore_wait(ready.at[side], 1)
                    copies[name].start()

                greeted.add(side)

        return early, late

    even_early, even_late = sender(even)
    odd_early, odd_late = sender(jnp.logical_not(even))

    def received(*some):
        for name in some:
            copies[name].wait_recv()

    def project(mu, v):
        at = window(v)
        field = load_spinor(psi, at)
        store_half(hm, mu, at, half(mu, field, -1.0))
        ahead = half(mu, field, 1.0)
        store_half(hp, mu, at, ahead)
        store_half(bl, mu, at, mat_vec(load_link(mu, at), ahead, True))

    def behind(v):
        at = window(v)
        store_half(hm, 2, at, half(2, load_spinor(psi, at), -1.0))

    inner = jnp.logical_not(first[Z_NEXT])
    arrived(0)
    for_each(chunks, behind)
    for name in ("c0", "c1"):
        pack(name, hm, 2)
    for name in ("c0", "c1"):
        pl.when(jnp.logical_and(inner, first[Z_PREV]))(copies[name].start)
    arrived(3)
    for_each(chunks, lambda v: project(2, v))
    for name in ("d0", "d1"):
        pack(name, bl, 2)
    pl.when(relay_high)(corners[0].start)
    even_early("d0")
    for name in ("c0", "d1"):
        pl.when(relay_high)(copies[name].start)
    for name in ("d1", "c0"):
        pl.when(jnp.logical_and(z_high, t_place == 0))(copies[name].start)
    arrived(4)
    for_each(chunks, lambda v: project(3, v))
    for name in ("a0", "a1"):
        pack(name, hm, 3)
    for name in ("b0", "b1"):
        pack(name, bl, 3)
    even_early("b0", "a0", "a1", "b1")
    even_late("b0", "b1")
    odd_early("a0", "b0", "a1", "b1", "d0")
    for c in range(18):
        link_out[c * line:(c + 1) * line, :] = link[36 + c, lines((0, z_last)), :]
    pl.when(relay_high)(corners[2].start)
    pl.when(jnp.logical_and(even, z_high))(copies["c1"].start)
    pl.when(jnp.logical_and(jnp.logical_not(even), z_high))(copies["c0"].start)

    arrived(1)
    for_each(chunks, lambda v: project(0, v))
    arrived(2)
    for_each(chunks, lambda v: project(1, v))

    for c in range(12):
        sh_hm[0, c] = shift_x1(hm[0, c], 1)
        sh_bl[0, c] = shift_x1(bl[0, c], -1)
        sh_hm[1, c] = shift_x2(hm[1, c], 1)
        sh_bl[1, c] = shift_x2(bl[1, c], -1)
        z_ahead(hm, sh_hm, c)
        z_behind(bl, sh_bl, c)
        t_ahead(hm, sh_hm, c)
        t_behind(bl, sh_bl, c)

    def hop(mu, at, total):
        ahead = mat_vec(load_link(mu, at), load_half(sh_hm, mu, at), False)
        store_half(prod, mu, at, ahead)
        total = add_whole(mu, total, ahead, -1.0)
        return add_whole(mu, total, load_half(sh_bl, mu, at), 1.0)

    zero = jnp.zeros((TILE, LANES), jnp.float32)

    def nothing():
        return [[(zero, zero)] * 3 for _ in range(4)]

    even_late("d0", "d1")
    odd_late("d0", "d1")
    arrived(5)

    def local(v):
        at = window(v)
        field = load_spinor(psi, at)
        total = nothing()
        for mu in (0, 1):
            total = hop(mu, at, total)
        for s in range(4):
            for c in range(3):
                base = 36 * (s // 2) + 6 * (3 * (s % 2) + c)
                re = (4.0 + bare_mass) * field[s][c][0] - 0.5 * total[s][c][0]
                im = (4.0 + bare_mass) * field[s][c][1] - 0.5 * total[s][c][1]
                for k in range(6):
                    other = field[2 * (s // 2) + k // 3][k % 3]
                    c_re = clov[base + k, at, :]
                    c_im = clov[72 + base + k, at, :]
                    re = re + (c_re * other[0] - c_im * other[1])
                    im = im + (c_re * other[1] + c_im * other[0])
                acc[3 * s + c, at, :] = re
                acc[12 + 3 * s + c, at, :] = im

    for_each(chunks, local)

    def with_hops(mu, at):
        total = hop(mu, at, nothing())
        held = load_spinor(acc, at)
        return [
            [(held[s][c][0] - 0.5 * total[s][c][0], held[s][c][1] - 0.5 * total[s][c][1]) for c in range(3)]
            for s in range(4)
        ]

    def partial(across, along, v):
        at = window(v)
        store_half(hphi, along, at, half(along, with_hops(across, at), 1.0))

    def signed(sign):
        return lambda value, at, c: value * sign

    low_chunks = -(-face_t // TILE)
    high_chunk = (rows - face_t) // TILE

    odd_early("d1")
    pl.when(jnp.logical_and(jnp.logical_not(even), z_high))(copies["c1"].start)
    odd_late("b0", "b1")
    for c in range(12):
        sh_bl[2, c, lines((0, 0)), :] = jnp.zeros((line, LANES), jnp.float32)
        sh_hm[2, c, lines((0, z_last)), :] = jnp.zeros((line, LANES), jnp.float32)

    def send_f(name, when):
        @pl.when(when)
        def _():
            for_each(low_chunks, lambda v: partial(2, 3, v))
            pack(name, hphi, 3)
            copies[name].start()

    send_f("f0", relay_low)
    send_f("f1", relay_high)

    @pl.when(jnp.logical_and(z_low, True))
    def _():
        pl.semaphore_wait(ready.at[Z_PREV], 1)
        pl.when(relay)(corners[1].start)
        copies["c0"].start()
        copies["c1"].start()

    even_late("a0", "a1")
    odd_late("a0", "a1")

    received("a0")
    unpack("a0", sh_hm, 3, signed(high_sign))
    for_each(chunks, lambda v: partial(3, 2, v), high_chunk)
    pack("e1", hphi, 2)
    copies["e1"].start()
    received("b0")
    unpack("b0", sh_bl, 3, signed(low_sign))
    for_each(-(-(rows - face_t) // TILE), lambda v: partial(3, 2, v))
    pack("e0", hphi, 2)
    copies["e0"].start()

    def take_c():
        received("c0")
        unpack("c0", sh_hm, 2)
        send_f("f1", jnp.logical_not(relay_high))

    def take_d():
        received("d0")
        unpack("d0", sh_bl, 2)
        send_f("f0", jnp.logical_not(relay_low))

    pl.when(jnp.logical_not(z_low))(take_d)
    take_c()
    pl.when(z_low)(take_d)

    received("a1", "b1")
    unpack("a1", sh_hm, 3, signed(high_sign))
    unpack("b1", sh_bl, 3, signed(low_sign))

    def gather(v):
        at = window(v)
        store_spinor(acc, at, with_hops(3, at))

    for_each(chunks, gather)
    received("c1", "d1")
    unpack("c1", sh_hm, 2)
    unpack("d1", sh_bl, 2)

    def finish(v):
        at = window(v)
        phi = with_hops(2, at)
        store_spinor(out_ref, at, phi)
        for mu in range(4):
            store_half(hphi, mu, at, half(mu, phi, 1.0))

    for_each(chunks, finish)

    for c in range(12):
        sh_hphi[0, c] = shift_x1(hphi[0, c], 1)
        sh_hphi[1, c] = shift_x2(hphi[1, c], 1)
        z_ahead(hphi, sh_hphi, c)
        t_ahead(hphi, sh_hphi, c)

    def force(mu, v):
        at = window(v)
        second = mat_vec(load_link(mu, at), load_half(sh_hphi, mu, at), False)
        second_right = load_half(hp, mu, at)
        first = load_half(prod, mu, at)
        first_right = half(mu, load_spinor(out_ref, at), -1.0)
        pairs = [(first[s], first_right[s]) for s in range(2)] + [(second[s], second_right[s]) for s in range(2)]

        def w_re(a, b):
            return csum([l[a][0] * r[b][0] + l[a][1] * r[b][1] for l, r in pairs])

        def w_im(a, b):
            return csum([l[a][1] * r[b][0] - l[a][0] * r[b][1] for l, r in pairs])

        diag = [w_im(a, a) for a in range(3)]
        third = (diag[0] + diag[1] + diag[2]) * (1.0 / 3.0)
        base = 18 * mu
        for a in range(3):
            force_ref[base + 4 * a, at, :] = zero
            force_ref[base + 9 + 4 * a, at, :] = diag[a] - third
            for b in range(a + 1, 3):
                re = 0.5 * (w_re(a, b) - w_re(b, a))
                im = 0.5 * (w_im(a, b) + w_im(b, a))
                force_ref[base + 3 * a + b, at, :] = re
                force_ref[base + 3 * b + a, at, :] = -re
                force_ref[base + 9 + 3 * a + b, at, :] = im
                force_ref[base + 9 + 3 * b + a, at, :] = im

    for mu in (0, 1):
        for_each(chunks, lambda v: force(mu, v))

    for name in ("f0", "f1"):
        received(name)
        unpack(name, sh_hphi, 3, lambda value, at, c: value * high_sign - bl[3, c, lines(at), :])

    def corner(k, c):
        return corner_in[k, c * line:(c + 1) * line, :]

    def corner_half(k):
        return [[(corner(k, 3 * s + c), corner(k, 6 + 3 * s + c)) for c in range(3)] for s in range(2)]

    none = [[(0.0, 0.0)] * 3 for _ in range(4)]

    def add_corner(value, sign, z):
        extra = half(3, add_whole(2, none, value, sign), 1.0)
        for s in range(2):
            for c in range(3):
                for n, part in enumerate(extra[s][c]):
                    place = 3, 6 * n + 3 * s + c, lines((t_last, z)), slice(None)
                    sh_hphi[place] = sh_hphi[place] - 0.5 * high_sign * part

    @pl.when(relayed_low)
    def _():
        corners[0].wait_recv()
        add_corner(corner_half(0), 1.0, 0)

    @pl.when(relayed_high)
    def _():
        corners[2].wait_recv()
        corners[1].wait_recv()
        near_link = [[(corner(2, 3 * a + b), corner(2, 9 + 3 * a + b)) for b in range(3)] for a in range(3)]
        add_corner(mat_vec(near_link, corner_half(1), False), -1.0, z_last)

    for_each(chunks, lambda v: force(3, v))
    for name in ("e0", "e1"):
        received(name)
        unpack(name, sh_hphi, 2, lambda value, at, c: value - bl[2, c, lines(at), :])
    for_each(chunks, lambda v: force(2, v))
    for name in names:
        copies[name].wait_send()
    for k, mine in enumerate((relay_high, relay_low, relay_high)):
        pl.when(mine)(corners[k].wait_send)


def body(spinor, links, clover):
    nt, nz = spinor.shape[3], spinor.shape[4]
    sites = spinor.shape[-3:]
    x, u, c = (a.reshape((-1,) + sites) for a in (spinor, links, clover))
    parts = nt * (sites[2] // LANES)
    rows = parts * nz
    assert nt > 1 and nz > 1
    line = rows // (nt * nz)
    face = max(nt - 1, nz - 1) * line

    def halves():
        return pltpu.VMEM((4, 12, rows, LANES), jnp.float32)

    def held(array):
        return pltpu.VMEM((array.shape[0], parts, nz, LANES), jnp.float32)

    phi, anti = pl.pallas_call(
        lambda *refs: kernel(nt, nz, *refs),
        name="wilson",
        out_shape=(
            pltpu.VMEM((24, parts, nz, LANES), jnp.float32),
            pltpu.VMEM((u.shape[0], parts, nz, LANES), jnp.float32),
        ),
        in_specs=[pl.BlockSpec(memory_space=pltpu.HBM)] * 3,
        out_specs=(pl.BlockSpec(memory_space=pltpu.VMEM),) * 2,
        scratch_shapes=[
            held(x), held(u), held(c),
            halves(), halves(), halves(), halves(), halves(), halves(),
            pltpu.VMEM((24, rows, LANES), jnp.float32),
            halves(), halves(),
            pltpu.VMEM((12, 12 * face, LANES), jnp.float32),
            pltpu.VMEM((12, 12 * face, LANES), jnp.float32),
            pltpu.VMEM((18 * line, LANES), jnp.float32),
            pltpu.VMEM((3, 18 * line, LANES), jnp.float32),
            pltpu.SemaphoreType.DMA((6,)),
            pltpu.SemaphoreType.DMA((15,)),
            pltpu.SemaphoreType.DMA((15,)),
            pltpu.SemaphoreType.REGULAR((4,)),
        ],
        compiler_params=pltpu.CompilerParams(collective_id=0, has_side_effects=True, vmem_limit_bytes=56 * 1024 * 1024),
    )(x, u, c)
    applied, force = pl.pallas_call(
        write_out,
        name="write_out",
        out_shape=(
            jax.ShapeDtypeStruct(x.shape, jnp.float32),
            jax.ShapeDtypeStruct(u.shape, jnp.float32),
        ),
        in_specs=[pl.BlockSpec(memory_space=pltpu.VMEM)] * 2,
        out_specs=(pl.BlockSpec(memory_space=pl.ANY),) * 2,
        scratch_shapes=[pltpu.SemaphoreType.DMA((2,))],
        compiler_params=pltpu.CompilerParams(vmem_limit_bytes=8 * 1024 * 1024),
    )(phi, anti)
    return applied.reshape(spinor.shape), force.reshape(links.shape)


def solution(mesh):
    return jax.shard_map(
        body,
        mesh=mesh,
        in_specs=(
            P(None, None, None, "ta", "gz", None),
            P(None, None, None, None, "ta", "gz", None),
            P(None, None, None, None, "ta", "gz", None),
        ),
        out_specs=(
            P(None, None, None, "ta", "gz", None),
            P(None, None, None, None, "ta", "gz", None),
        ),
        check_vma=False,
    )
```

```python
import jax
import jax.numpy as jnp
from jax import lax
from jax.experimental import pallas as pl
from jax.experimental.pallas import tpu as pltpu
from jax.sharding import PartitionSpec as P

NX = 64
LANES = 128
TILE = 8
MESH = pl.DeviceIdType.MESH

bare_mass = -0.25
gamma_table = (
    ((3, 0.0, -1.0), (2, 0.0, -1.0), (1, 0.0, 1.0), (0, 0.0, 1.0)),
    ((3, -1.0, 0.0), (2, 1.0, 0.0), (1, 1.0, 0.0), (0, -1.0, 0.0)),
    ((2, 0.0, -1.0), (3, 0.0, 1.0), (0, 0.0, 1.0), (1, 0.0, -1.0)),
    ((2, 1.0, 0.0), (3, 1.0, 0.0), (0, 1.0, 0.0), (1, 1.0, 0.0)),
)


def add_signed(a, b, positive):
    return a + b if positive else a - b


def add_phase(a, b, phase_re, phase_im):
    if phase_im == 0.0:
        up = phase_re > 0
        return (add_signed(a[0], b[0], up), add_signed(a[1], b[1], up))
    up = phase_im > 0
    return (add_signed(a[0], b[1], not up), add_signed(a[1], b[0], up))


def half(mu, field, sign):
    out = []
    for s in range(2):
        source, p_re, p_im = gamma_table[mu][s]
        out.append(
            [add_phase(field[s][c], field[source][c], sign * p_re, sign * p_im) for c in range(3)]
        )
    return out


def add_whole(mu, total, halves, sign):
    out = [[add_phase(total[s][c], halves[s][c], 1.0, 0.0) for c in range(3)] for s in range(2)]
    for s in (2, 3):
        source, p_re, p_im = gamma_table[mu][s]
        out.append(
            [add_phase(total[s][c], halves[source][c], sign * p_re, sign * p_im) for c in range(3)]
        )
    return out


def csum(terms):
    total = terms[0]
    for term in terms[1:]:
        total = total + term
    return total


def mat_vec(link, vec, dagger):
    out = []
    for s in range(2):
        rows = []
        for a in range(3):
            re, im = [], []
            for b in range(3):
                h = vec[s][b]
                if dagger:
                    m = link[b][a]
                    re.append(m[0] * h[0] + m[1] * h[1])
                    im.append(m[0] * h[1] - m[1] * h[0])
                else:
                    m = link[a][b]
                    re.append(m[0] * h[0] - m[1] * h[1])
                    im.append(m[0] * h[1] + m[1] * h[0])
            rows.append((csum(re), csum(im)))
        out.append(rows)
    return out


def flat(ref):
    return ref.reshape(ref.shape[0], ref.shape[1] * ref.shape[2] * ref.shape[3], ref.shape[4])


def for_each(count, body, low=0):
    def step(i, carry):
        body(i)
        return carry

    lax.fori_loop(low, count, step, 0)


def window(v):
    return pl.ds(pl.multiple_of(v * TILE, TILE), TILE)


def load_spinor(ref, at):
    return [[(ref[3 * s + c, at, :], ref[12 + 3 * s + c, at, :]) for c in range(3)] for s in range(4)]


def load_half(ref, mu, at):
    return [[(ref[mu, 3 * s + c, at, :], ref[mu, 6 + 3 * s + c, at, :]) for c in range(3)] for s in range(2)]


def load_link(ref, mu, at):
    return [[(ref[18 * mu + 3 * a + b, at, :], ref[18 * mu + 9 + 3 * a + b, at, :]) for b in range(3)] for a in range(3)]


def force_of(mu, v, phi, link, hp, prod, hphi, force_ref):
    at = window(v)
    zero = jnp.zeros((TILE, LANES), jnp.float32)
    second = mat_vec(load_link(link, mu, at), load_half(hphi, mu, at), False)
    second_right = load_half(hp, mu, at)
    first = load_half(prod, mu, at)
    first_right = half(mu, load_spinor(phi, at), -1.0)
    pairs = [(first[s], first_right[s]) for s in range(2)] + [(second[s], second_right[s]) for s in range(2)]

    def w_re(a, b):
        return csum([l[a][0] * r[b][0] + l[a][1] * r[b][1] for l, r in pairs])

    def w_im(a, b):
        return csum([l[a][1] * r[b][0] - l[a][0] * r[b][1] for l, r in pairs])

    diag = [w_im(a, a) for a in range(3)]
    third = (diag[0] + diag[1] + diag[2]) * (1.0 / 3.0)
    base = 18 * mu
    for a in range(3):
        force_ref[base + 4 * a, at, :] = zero
        force_ref[base + 9 + 4 * a, at, :] = diag[a] - third
        for b in range(a + 1, 3):
            re = 0.5 * (w_re(a, b) - w_re(b, a))
            im = 0.5 * (w_im(a, b) + w_im(b, a))
            force_ref[base + 3 * a + b, at, :] = re
            force_ref[base + 3 * b + a, at, :] = -re
            force_ref[base + 9 + 3 * a + b, at, :] = im
            force_ref[base + 9 + 3 * b + a, at, :] = im


def finish_kernel(phi_in, early_in, link_in, hp, prod, hphi, phi_hbm, force_hbm, late, sem):
    phi, link = flat(phi_in), flat(link_in)
    count = early_in.shape[0]
    pltpu.make_async_copy(early_in, force_hbm.at[pl.ds(0, count)], sem.at[0]).start()
    pltpu.make_async_copy(phi_in, phi_hbm, sem.at[1]).start()
    for mu in (3, 2):
        for_each(phi.shape[1] // TILE, lambda v: force_of(mu, v, phi, link, hp, prod, hphi, flat(late)))
        part = pl.ds(18 * mu, 18)
        pltpu.make_async_copy(late.at[part], force_hbm.at[part], sem.at[0]).start()
    pltpu.make_async_copy(phi_in, phi_hbm, sem.at[1]).wait()
    pltpu.make_async_copy(late, force_hbm, sem.at[0]).wait()


def kernel(nt, nz, x_hbm, u_hbm, c_hbm, phi_out, force_out, link_in, hp, prod, sh_hphi, psi_in, clov_in, hm, bl,
           sh_hm, sh_bl, acc, hphi, face_out, face_in, link_out, corner_in, in_sem,
           send_sem, recv_sem, ready):
    psi, link, clov, out_ref, force_ref = map(flat, (psi_in, link_in, clov_in, phi_out, force_out))
    rows = psi.shape[1]
    face_t = rows // nt
    face_z = rows // nz
    line = face_t // nz
    chunks = rows // TILE
    t_place, z_place = lax.axis_index("ta"), lax.axis_index("gz")
    t_count, z_count = lax.axis_size("ta"), lax.axis_size("gz")
    low_sign = jnp.where(t_place == 0, -1.0, 1.0).astype(jnp.float32)
    high_sign = jnp.where(t_place == t_count - 1, -1.0, 1.0).astype(jnp.float32)

    T_PREV, T_NEXT, Z_PREV, Z_NEXT = range(4)
    near = (
        (lax.rem(t_place + t_count - 1, t_count), z_place),
        (lax.rem(t_place + 1, t_count), z_place),
        (t_place, lax.rem(z_place + z_count - 1, z_count)),
        (t_place, lax.rem(z_place + 1, z_count)),
    )
    first = (t_place > 0, t_place == t_count - 1, z_place > 0, z_place == z_count - 1)
    barrier = pltpu.get_barrier_semaphore()

    groups = [(x_hbm, psi_in)]
    for part in (pl.ds(36, 18), pl.ds(54, 18), pl.ds(0, 36)):
        groups.append((u_hbm.at[part], link_in.at[part]))
    groups.append((c_hbm, clov_in))

    def fetch(n):
        pltpu.make_async_copy(*groups[n], in_sem.at[n]).start()

    def arrived(n):
        pltpu.make_async_copy(*groups[n], in_sem.at[n]).wait()

    even = lax.rem(t_place, 2) == 0
    relay = jnp.logical_and(even, t_place > 0)
    t_after = near[T_NEXT][0]
    relayed = jnp.logical_and(lax.rem(t_after, 2) == 0, t_after > 0)
    z_low, z_high = z_place == 0, z_place == z_count - 1

    def greet(k, when):
        @pl.when(jnp.logical_and(when, jnp.logical_not(first[k])))
        def _():
            pl.semaphore_signal(barrier, inc=1, device_id=near[k], device_id_type=MESH)

    after = {Z_PREV: relay, T_PREV: jnp.logical_and(t_place == 0, z_place == 1)}
    for k in range(4):
        greet(k, jnp.logical_not(after[k]) if k in after else True)

    for n in (0, 1, 2):
        fetch(n)
    greeters = sum(f.astype(jnp.int32) for f in first)

    @pl.when(greeters > 0)
    def _():
        pl.semaphore_wait(barrier, greeters)

    for k, when in after.items():
        greet(k, when)
    for k in range(4):
        @pl.when(first[k])
        def _():
            pl.semaphore_signal(ready.at[k ^ 1], inc=1, device_id=near[k], device_id_type=MESH)
    for n in (3, 4):
        fetch(n)

    def store_spinor(ref, at, value):
        for s in range(4):
            for c in range(3):
                ref[3 * s + c, at, :] = value[s][c][0]
                ref[12 + 3 * s + c, at, :] = value[s][c][1]

    def store_half(ref, mu, at, value):
        for s in range(2):
            for c in range(3):
                ref[mu, 3 * s + c, at, :] = value[s][c][0]
                ref[mu, 6 + 3 * s + c, at, :] = value[s][c][1]

    lane = lax.broadcasted_iota(jnp.int32, (rows, LANES), 1)
    row = lax.broadcasted_iota(jnp.int32, (rows, LANES), 0)
    lane_in = lax.rem(lane, NX)
    row_in = lax.rem(row, face_t)
    upper = lane >= NX

    def shift_x1(value, step):
        if step == 1:
            near, far = pltpu.roll(value, LANES - 1, 1), pltpu.roll(value, NX - 1, 1)
            return jnp.where(lane_in == NX - 1, far, near)
        near, far = pltpu.roll(value, 1, 1), pltpu.roll(value, LANES - NX + 1, 1)
        return jnp.where(lane_in == 0, far, near)

    def shift_x2(value, step):
        turned = pltpu.roll(value, NX, 1)
        if step == 1:
            near = pltpu.roll(turned, rows - nz, 0)
            far = pltpu.roll(turned, face_t - nz, 0)
            moved = jnp.where(row_in >= face_t - nz, far, near)
            return jnp.where(upper, moved, turned)
        near = pltpu.roll(turned, nz, 0)
        far = pltpu.roll(turned, rows - face_t + nz, 0)
        moved = jnp.where(row_in < nz, far, near)
        return jnp.where(upper, turned, moved)

    def z_ahead(src, dst, c):
        for z in range(nz - 1):
            dst[2, c, pl.ds(z, face_z, nz), :] = src[2, c, pl.ds(z + 1, face_z, nz), :]

    def z_behind(src, dst, c):
        for z in range(1, nz):
            dst[2, c, pl.ds(z, face_z, nz), :] = src[2, c, pl.ds(z - 1, face_z, nz), :]

    def t_ahead(src, dst, c):
        dst[3, c, pl.ds(0, rows - face_t), :] = src[3, c, pl.ds(face_t, rows - face_t), :]

    def t_behind(src, dst, c):
        dst[3, c, pl.ds(face_t, rows - face_t), :] = src[3, c, pl.ds(0, rows - face_t), :]

    t_last, z_last = nt - 1, nz - 1
    messages = {
        "a0": (T_PREV, [(0, 0)], [(t_last, 0)]),
        "a1": (T_PREV, [(0, z) for z in range(1, nz)], [(t_last, z) for z in range(1, nz)]),
        "b0": (T_NEXT, [(t_last, 0)], [(0, 0)]),
        "b1": (T_NEXT, [(t_last, z) for z in range(1, nz)], [(0, z) for z in range(1, nz)]),
        "c0": (Z_PREV, [(0, 0)], [(0, z_last)]),
        "c1": (Z_PREV, [(t, 0) for t in range(1, nt)], [(t, z_last) for t in range(1, nt)]),
        "d0": (Z_NEXT, [(0, z_last)], [(0, 0)]),
        "d1": (Z_NEXT, [(t, z_last) for t in range(1, nt)], [(t, 0) for t in range(1, nt)]),
        "e0": (Z_PREV, [(t, 0) for t in range(t_last)], [(t, z_last) for t in range(t_last)]),
        "e1": (Z_PREV, [(t_last, 0)], [(t_last, z_last)]),
        "f0": (T_PREV, [(0, z) for z in range(z_last)], [(t_last, z) for z in range(z_last)]),
        "f1": (T_PREV, [(0, z_last)], [(t_last, z_last)]),
    }
    names = list(messages)

    def place(name, i, c):
        return names.index(name), pl.ds((12 * i + c) * line, line)

    def lines(at):
        return pl.ds(at[0] * face_t + at[1], line, nz)

    def pack(name, src, mu):
        for i, at in enumerate(messages[name][1]):
            for c in range(12):
                k, held = place(name, i, c)
                face_out[k, held, :] = src[mu, c, lines(at), :]

    def unpack(name, dst, mu, change=lambda value, at, c: value):
        for i, at in enumerate(messages[name][2]):
            for c in range(12):
                k, held = place(name, i, c)
                dst[mu, c, lines(at), :] = change(face_in[k, held, :], at, c)

    together = ("a0", "b0", "c0", "d0", "a1 b1", "c1 d1", "e0 e1 f0 f1")
    home = {name: n for n, some in enumerate(together) for name in some.split()}
    sizes = {name: 12 * line * len(messages[name][1]) for name in names}

    def copy_of(name):
        k, size = names.index(name), pl.ds(0, sizes[name])
        return pltpu.make_async_remote_copy(
            src_ref=face_out.at[k, size], dst_ref=face_in.at[k, size], send_sem=send_sem.at[0],
            recv_sem=recv_sem.at[home[name]], device_id=near[messages[name][0]], device_id_type=MESH,
        )

    copies = {name: copy_of(name) for name in names}

    def await_rows(count, sem):
        held = face_in.reshape(face_in.shape[0] * face_in.shape[1], LANES).at[pl.ds(0, count)]
        pltpu.make_async_copy(held, held, sem).wait()

    CORNER = len(together)

    def corner_of(k, held, target):
        size = pl.ds(0, held.shape[0])
        return pltpu.make_async_remote_copy(
            src_ref=held, dst_ref=corner_in.at[k, size], send_sem=send_sem.at[1],
            recv_sem=recv_sem.at[CORNER], device_id=target, device_id_type=MESH,
        )

    t_before = near[T_PREV][0]
    corners = [
        corner_of(0, face_out.at[names.index("d0"), pl.ds(0, 12 * line)], (t_before, near[Z_NEXT][1])),
        corner_of(1, face_out.at[names.index("c0"), pl.ds(0, 12 * line)], (t_before, near[Z_PREV][1])),
        corner_of(2, link_out, near[T_PREV]),
        corner_of(0, face_out.at[names.index("b0"), pl.ds(0, 12 * line)], (near[T_NEXT][0], near[Z_PREV][1])),
    ]
    edge = jnp.logical_and(t_place == 0, z_place == 1)
    edge_from = jnp.logical_and(t_place == t_count - 1, z_place == 1)
    edge_to = jnp.logical_and(t_place == 0, z_low)
    relay_high, relay_low = jnp.logical_and(relay, z_high), jnp.logical_and(relay, z_low)
    relayed_high, relayed_low = jnp.logical_and(relayed, z_high), jnp.logical_and(relayed, z_low)
    def sender(mine):
        greeted = set()

        def early(*some):
            for name in some:
                pl.when(jnp.logical_and(mine, first[messages[name][0]]))(copies[name].start)

        def late(*some):
            for name in some:
                side = messages[name][0]

                @pl.when(jnp.logical_and(mine, jnp.logical_not(first[side])))
                def _():
                    if side not in greeted:
                        pl.semaphore_wait(ready.at[side], 1)
                    copies[name].start()

                greeted.add(side)

        return early, late

    even_early, even_late = sender(even)
    odd_early, odd_late = sender(jnp.logical_not(even))

    def received(*some):
        assert set(some) == {name for name in names if home[name] == home[some[0]]}
        await_rows(sum(sizes[name] for name in some), recv_sem.at[home[some[0]]])

    def project(mu, v):
        at = window(v)
        field = load_spinor(psi, at)
        store_half(hm, mu, at, half(mu, field, -1.0))
        ahead = half(mu, field, 1.0)
        store_half(hp, mu, at, ahead)
        store_half(bl, mu, at, mat_vec(load_link(link, mu, at), ahead, True))

    def behind(v):
        at = window(v)
        store_half(hm, 2, at, half(2, load_spinor(psi, at), -1.0))

    inner = jnp.logical_not(first[Z_NEXT])
    arrived(0)
    for_each(chunks, behind)
    for name in ("c0", "c1"):
        pack(name, hm, 2)
    for name in ("c0", "c1"):
        pl.when(jnp.logical_and(inner, first[Z_PREV]))(copies[name].start)
    arrived(1)
    for_each(chunks, lambda v: project(2, v))
    for name in ("d0", "d1"):
        pack(name, bl, 2)
    pl.when(relay_high)(corners[0].start)
    even_early("d0")
    for name in ("c0", "d1"):
        pl.when(relay_high)(copies[name].start)
    for name in ("d1", "c0"):
        pl.when(jnp.logical_and(z_high, t_place == 0))(copies[name].start)
    arrived(2)
    for_each(chunks, lambda v: project(3, v))
    for name in ("a0", "a1"):
        pack(name, hm, 3)
    for name in ("b0", "b1"):
        pack(name, bl, 3)
    even_early("b0", "a0", "a1", "b1")
    even_late("b0", "b1")
    pl.when(edge_from)(corners[3].start)
    odd_early("a0", "b0", "a1", "b1", "d0")
    for c in range(18):
        link_out[c * line:(c + 1) * line, :] = link[36 + c, lines((0, z_last)), :]
    pl.when(relay_high)(corners[2].start)
    pl.when(jnp.logical_and(even, z_high))(copies["c1"].start)
    pl.when(jnp.logical_and(jnp.logical_not(even), z_high))(copies["c0"].start)

    arrived(3)
    for_each(chunks, lambda v: project(0, v))
    for_each(chunks, lambda v: project(1, v))

    for c in range(12):
        sh_hm[0, c] = shift_x1(hm[0, c], 1)
        sh_bl[0, c] = shift_x1(bl[0, c], -1)
        sh_hm[1, c] = shift_x2(hm[1, c], 1)
        sh_bl[1, c] = shift_x2(bl[1, c], -1)
        z_ahead(hm, sh_hm, c)
        z_behind(bl, sh_bl, c)
        t_ahead(hm, sh_hm, c)
        t_behind(bl, sh_bl, c)

    def hop(mu, at, total):
        ahead = mat_vec(load_link(link, mu, at), load_half(sh_hm, mu, at), False)
        store_half(prod, mu, at, ahead)
        total = add_whole(mu, total, ahead, -1.0)
        return add_whole(mu, total, load_half(sh_bl, mu, at), 1.0)

    zero = jnp.zeros((TILE, LANES), jnp.float32)

    def nothing():
        return [[(zero, zero)] * 3 for _ in range(4)]

    even_late("d0", "d1")
    odd_late("d0", "d1")
    arrived(4)

    def local(v):
        at = window(v)
        field = load_spinor(psi, at)
        total = nothing()
        for mu in (0, 1):
            total = hop(mu, at, total)
        for s in range(4):
            for c in range(3):
                base = 36 * (s // 2) + 6 * (3 * (s % 2) + c)
                re = (4.0 + bare_mass) * field[s][c][0] - 0.5 * total[s][c][0]
                im = (4.0 + bare_mass) * field[s][c][1] - 0.5 * total[s][c][1]
                for k in range(6):
                    other = field[2 * (s // 2) + k // 3][k % 3]
                    c_re = clov[base + k, at, :]
                    c_im = clov[72 + base + k, at, :]
                    re = re + (c_re * other[0] - c_im * other[1])
                    im = im + (c_re * other[1] + c_im * other[0])
                acc[3 * s + c, at, :] = re
                acc[12 + 3 * s + c, at, :] = im

    for_each(chunks, local)

    def with_hops(mu, at):
        total = hop(mu, at, nothing())
        held = load_spinor(acc, at)
        return [
            [(held[s][c][0] - 0.5 * total[s][c][0], held[s][c][1] - 0.5 * total[s][c][1]) for c in range(3)]
            for s in range(4)
        ]

    def partial(across, along, v):
        at = window(v)
        store_half(hphi, along, at, half(along, with_hops(across, at), 1.0))

    def signed(sign):
        return lambda value, at, c: value * sign

    low_chunks = -(-face_t // TILE)
    high_chunk = (rows - face_t) // TILE

    odd_early("d1")
    pl.when(jnp.logical_and(jnp.logical_not(even), z_high))(copies["c1"].start)
    odd_late("b0", "b1")
    for c in range(12):
        sh_bl[2, c, lines((0, 0)), :] = jnp.zeros((line, LANES), jnp.float32)
        sh_hm[2, c, lines((0, z_last)), :] = jnp.zeros((line, LANES), jnp.float32)

    def send_f(name, when):
        @pl.when(when)
        def _():
            for_each(low_chunks, lambda v: partial(2, 3, v))
            pack(name, hphi, 3)
            copies[name].start()

    send_f("f0", relay_low)
    send_f("f1", relay_high)

    @pl.when(jnp.logical_and(z_low, True))
    def _():
        pl.semaphore_wait(ready.at[Z_PREV], 1)
        pl.when(relay)(corners[1].start)
        copies["c0"].start()
        copies["c1"].start()

    even_late("a0", "a1")
    odd_late("a0", "a1")

    def send_e(name):
        low, high = (high_chunk, chunks) if name == "e1" else (0, -(-(rows - face_t) // TILE))
        for_each(high, lambda v: partial(3, 2, v), low)
        pack(name, hphi, 2)
        copies[name].start()

    def take_a():
        received("a0")
        unpack("a0", sh_hm, 3, signed(high_sign))
        send_e("e1")

    def take_b():
        received("b0")
        unpack("b0", sh_bl, 3, signed(low_sign))
        pl.when(jnp.logical_not(edge))(lambda: send_e("e0"))

    @pl.when(edge)
    def _():
        for c in range(12):
            sh_bl[3, c, lines((0, 0)), :] = jnp.zeros((line, LANES), jnp.float32)
        send_e("e0")

    pl.when(jnp.logical_not(even))(take_b)
    take_a()
    pl.when(even)(take_b)

    def take_c():
        received("c0")
        unpack("c0", sh_hm, 2)
        send_f("f1", jnp.logical_not(relay_high))

    def take_d():
        received("d0")
        unpack("d0", sh_bl, 2)
        send_f("f0", jnp.logical_not(relay_low))

    pl.when(jnp.logical_not(z_low))(take_d)
    take_c()
    pl.when(z_low)(take_d)

    received("a1", "b1")
    unpack("a1", sh_hm, 3, signed(high_sign))
    unpack("b1", sh_bl, 3, signed(low_sign))

    def gather(v):
        at = window(v)
        store_spinor(acc, at, with_hops(3, at))

    for_each(chunks, gather)
    received("c1", "d1")
    unpack("c1", sh_hm, 2)
    unpack("d1", sh_bl, 2)

    def finish(v):
        at = window(v)
        phi = with_hops(2, at)
        store_spinor(out_ref, at, phi)
        for mu in range(4):
            store_half(hphi, mu, at, half(mu, phi, 1.0))

    for_each(chunks, finish)

    for c in range(12):
        sh_hphi[0, c] = shift_x1(hphi[0, c], 1)
        sh_hphi[1, c] = shift_x2(hphi[1, c], 1)
        z_ahead(hphi, sh_hphi, c)
        t_ahead(hphi, sh_hphi, c)

    for mu in (0, 1):
        for_each(chunks, lambda v: force_of(mu, v, out_ref, link, hp, prod, sh_hphi, force_ref))

    received("e0", "e1", "f0", "f1")
    for name in ("f0", "f1"):
        unpack(name, sh_hphi, 3, lambda value, at, c: value * high_sign - bl[3, c, lines(at), :])
    for name in ("e0", "e1"):
        unpack(name, sh_hphi, 2, lambda value, at, c: value - bl[2, c, lines(at), :])

    def corner(k, c):
        return corner_in[k, c * line:(c + 1) * line, :]

    def corner_half(k):
        return [[(corner(k, 3 * s + c), corner(k, 6 + 3 * s + c)) for c in range(3)] for s in range(2)]

    none = [[(0.0, 0.0)] * 3 for _ in range(4)]

    def add_corner(across, along, value, sign, at, factor):
        extra = half(along, add_whole(across, none, value, sign), 1.0)
        for s in range(2):
            for c in range(3):
                for n, part in enumerate(extra[s][c]):
                    place = along, 6 * n + 3 * s + c, lines(at), slice(None)
                    sh_hphi[place] = sh_hphi[place] - 0.5 * factor * part

    @pl.when(relayed_low)
    def _():
        await_rows(12 * line, recv_sem.at[CORNER])
        add_corner(2, 3, corner_half(0), 1.0, (t_last, 0), high_sign)

    @pl.when(relayed_high)
    def _():
        await_rows(30 * line, recv_sem.at[CORNER])
        near_link = [[(corner(2, 3 * a + b), corner(2, 9 + 3 * a + b)) for b in range(3)] for a in range(3)]
        add_corner(2, 3, mat_vec(near_link, corner_half(1), False), -1.0, (t_last, z_last), high_sign)

    @pl.when(edge_to)
    def _():
        await_rows(12 * line, recv_sem.at[CORNER])
        add_corner(3, 2, corner_half(0), 1.0, (0, z_last), low_sign)

    await_rows(sum(sizes.values()), send_sem.at[0])
    for mine, count in ((relay_high, 30), (jnp.logical_or(relay_low, edge_from), 12)):
        pl.when(mine)(lambda: await_rows(count * line, send_sem.at[1]))


def body(spinor, links, clover):
    nt, nz, plane = spinor.shape[-3:]
    pieces = plane // LANES

    def tiled(a):
        return a.reshape(-1, nt, nz, pieces, LANES).transpose(0, 1, 3, 2, 4)

    def untiled(a, shape):
        return a.transpose(0, 1, 3, 2, 4).reshape(shape)

    x, u, c = map(tiled, (spinor, links, clover))
    rows = nt * pieces * nz
    assert nt > 1 and nz > 1
    line = rows // (nt * nz)
    face = max(nt - 1, nz - 1) * line

    def halves():
        return pltpu.VMEM((4, 12, rows, LANES), jnp.float32)

    def held(array):
        return pltpu.VMEM(array.shape, jnp.float32)

    made = pl.pallas_call(
        lambda *refs: kernel(nt, nz, *refs),
        name="wilson",
        out_shape=(held(x), held(u[:36]), held(u), halves(), halves(), halves()),
        in_specs=[pl.BlockSpec(memory_space=pltpu.HBM)] * 3,
        out_specs=(pl.BlockSpec(memory_space=pltpu.VMEM),) * 6,
        scratch_shapes=[
            held(x), held(c),
            halves(), halves(), halves(), halves(),
            pltpu.VMEM((24, rows, LANES), jnp.float32),
            halves(),
            pltpu.VMEM((12, 12 * face, LANES), jnp.float32),
            pltpu.VMEM((12, 12 * face, LANES), jnp.float32),
            pltpu.VMEM((18 * line, LANES), jnp.float32),
            pltpu.VMEM((3, 18 * line, LANES), jnp.float32),
            pltpu.SemaphoreType.DMA((5,)),
            pltpu.SemaphoreType.DMA((2,)),
            pltpu.SemaphoreType.DMA((8,)),
            pltpu.SemaphoreType.REGULAR((4,)),
        ],
        compiler_params=pltpu.CompilerParams(
            collective_id=0, has_side_effects=True, vmem_limit_bytes=54 * 1024 * 1024
        ),
    )(x, u, c)
    applied, force = pl.pallas_call(
        finish_kernel,
        name="finish",
        out_shape=(
            jax.ShapeDtypeStruct(x.shape, jnp.float32),
            jax.ShapeDtypeStruct(u.shape, jnp.float32),
        ),
        in_specs=[pl.BlockSpec(memory_space=pltpu.VMEM)] * 6,
        out_specs=(pl.BlockSpec(memory_space=pl.ANY),) * 2,
        scratch_shapes=[held(u), pltpu.SemaphoreType.DMA((2,))],
        compiler_params=pltpu.CompilerParams(vmem_limit_bytes=8 * 1024 * 1024),
    )(*made)
    return untiled(applied, spinor.shape), untiled(force, links.shape)


def solution(mesh):
    return jax.shard_map(
        body,
        mesh=mesh,
        in_specs=(
            P(None, None, None, "ta", "gz", None),
            P(None, None, None, None, "ta", "gz", None),
            P(None, None, None, None, "ta", "gz", None),
        ),
        out_specs=(
            P(None, None, None, "ta", "gz", None),
            P(None, None, None, None, "ta", "gz", None),
        ),
        check_vma=False,
    )
```

```python
import jax
import jax.numpy as jnp
from jax import lax
from jax.experimental import pallas as pl
from jax.experimental.pallas import tpu as pltpu
from jax.sharding import PartitionSpec as P

NX = 64
LANES = 128
TILE = 8
MESH = pl.DeviceIdType.MESH

bare_mass = -0.25
gamma_table = (
    ((3, 0.0, -1.0), (2, 0.0, -1.0), (1, 0.0, 1.0), (0, 0.0, 1.0)),
    ((3, -1.0, 0.0), (2, 1.0, 0.0), (1, 1.0, 0.0), (0, -1.0, 0.0)),
    ((2, 0.0, -1.0), (3, 0.0, 1.0), (0, 0.0, 1.0), (1, 0.0, -1.0)),
    ((2, 1.0, 0.0), (3, 1.0, 0.0), (0, 1.0, 0.0), (1, 1.0, 0.0)),
)


def add_signed(a, b, positive):
    return a + b if positive else a - b


def add_phase(a, b, phase_re, phase_im):
    if phase_im == 0.0:
        up = phase_re > 0
        return (add_signed(a[0], b[0], up), add_signed(a[1], b[1], up))
    up = phase_im > 0
    return (add_signed(a[0], b[1], not up), add_signed(a[1], b[0], up))


def half(mu, field, sign):
    out = []
    for s in range(2):
        source, p_re, p_im = gamma_table[mu][s]
        out.append(
            [add_phase(field[s][c], field[source][c], sign * p_re, sign * p_im) for c in range(3)]
        )
    return out


def add_whole(mu, total, halves, sign):
    out = [[add_phase(total[s][c], halves[s][c], 1.0, 0.0) for c in range(3)] for s in range(2)]
    for s in (2, 3):
        source, p_re, p_im = gamma_table[mu][s]
        out.append(
            [add_phase(total[s][c], halves[source][c], sign * p_re, sign * p_im) for c in range(3)]
        )
    return out


def csum(terms):
    total = terms[0]
    for term in terms[1:]:
        total = total + term
    return total


def mat_vec(link, vec, dagger):
    out = []
    for s in range(2):
        rows = []
        for a in range(3):
            re, im = [], []
            for b in range(3):
                h = vec[s][b]
                if dagger:
                    m = link[b][a]
                    re.append(m[0] * h[0] + m[1] * h[1])
                    im.append(m[0] * h[1] - m[1] * h[0])
                else:
                    m = link[a][b]
                    re.append(m[0] * h[0] - m[1] * h[1])
                    im.append(m[0] * h[1] + m[1] * h[0])
            rows.append((csum(re), csum(im)))
        out.append(rows)
    return out


def flat(ref):
    return ref.reshape(ref.shape[0], ref.shape[1] * ref.shape[2] * ref.shape[3], ref.shape[4])


def for_each(count, body, low=0):
    def step(i, carry):
        body(i)
        return carry

    lax.fori_loop(low, count, step, 0)


def window(v):
    return pl.ds(pl.multiple_of(v * TILE, TILE), TILE)


def load_spinor(ref, at):
    return [[(ref[3 * s + c, at, :], ref[12 + 3 * s + c, at, :]) for c in range(3)] for s in range(4)]


def load_half(ref, mu, at):
    return [[(ref[mu, 3 * s + c, at, :], ref[mu, 6 + 3 * s + c, at, :]) for c in range(3)] for s in range(2)]


def load_link(ref, mu, at):
    return [[(ref[18 * mu + 3 * a + b, at, :], ref[18 * mu + 9 + 3 * a + b, at, :]) for b in range(3)] for a in range(3)]


def force_of(mu, v, phi, link, hp, prod, hphi, force_ref, base):
    at = window(v)
    zero = jnp.zeros((TILE, LANES), jnp.float32)
    second = mat_vec(load_link(link, mu, at), load_half(hphi, mu, at), False)
    second_right = load_half(hp, mu, at)
    first = load_half(prod, mu, at)
    first_right = half(mu, load_spinor(phi, at), -1.0)
    pairs = [(first[s], first_right[s]) for s in range(2)] + [(second[s], second_right[s]) for s in range(2)]

    def w_re(a, b):
        return csum([l[a][0] * r[b][0] + l[a][1] * r[b][1] for l, r in pairs])

    def w_im(a, b):
        return csum([l[a][1] * r[b][0] - l[a][0] * r[b][1] for l, r in pairs])

    diag = [w_im(a, a) for a in range(3)]
    third = (diag[0] + diag[1] + diag[2]) * (1.0 / 3.0)
    for a in range(3):
        force_ref[base + 4 * a, at, :] = zero
        force_ref[base + 9 + 4 * a, at, :] = diag[a] - third
        for b in range(a + 1, 3):
            re = 0.5 * (w_re(a, b) - w_re(b, a))
            im = 0.5 * (w_im(a, b) + w_im(b, a))
            force_ref[base + 3 * a + b, at, :] = re
            force_ref[base + 3 * b + a, at, :] = -re
            force_ref[base + 9 + 3 * a + b, at, :] = im
            force_ref[base + 9 + 3 * b + a, at, :] = im


def finish_kernel(phi_in, early_in, link_in, hp, prod, hphi, phi_hbm, force_hbm, late, sem):
    phi, link = flat(phi_in), flat(link_in)
    corner = jnp.logical_and(lax.axis_index("ta") == 0, lax.axis_index("gz") == 0)

    def write(held, mu, count=1):
        pltpu.make_async_copy(held, force_hbm.at[pl.ds(18 * mu, 18 * count)], sem.at[0]).start()

    def compute(mu, base):
        for_each(
            phi.shape[1] // TILE, lambda v: force_of(mu, v, phi, link, hp, prod, hphi, flat(late), base)
        )
        write(late.at[pl.ds(base, 18)], mu)

    write(early_in.at[pl.ds(0, 36)], 0, 2)
    applied = pltpu.make_async_copy(phi_in, phi_hbm, sem.at[1])
    applied.start()
    pl.when(corner)(lambda: write(early_in.at[pl.ds(36, 18)], 3))
    pl.when(jnp.logical_not(corner))(lambda: compute(3, 18))
    compute(2, 0)
    applied.wait()
    pltpu.make_async_copy(force_hbm, force_hbm, sem.at[0]).wait()


def kernel(nt, nz, x_hbm, u_hbm, c_hbm, phi_out, force_out, link_in, hp, prod, sh_hphi, psi_in, clov_in, hm, bl,
           sh_hm, sh_bl, acc, hphi, face_out, face_in, link_out, corner_in, in_sem,
           send_sem, recv_sem, ready):
    psi, link, clov, out_ref, force_ref = map(flat, (psi_in, link_in, clov_in, phi_out, force_out))
    rows = psi.shape[1]
    face_t = rows // nt
    face_z = rows // nz
    line = face_t // nz
    chunks = rows // TILE
    t_place, z_place = lax.axis_index("ta"), lax.axis_index("gz")
    t_count, z_count = lax.axis_size("ta"), lax.axis_size("gz")
    low_sign = jnp.where(t_place == 0, -1.0, 1.0).astype(jnp.float32)
    high_sign = jnp.where(t_place == t_count - 1, -1.0, 1.0).astype(jnp.float32)

    T_PREV, T_NEXT, Z_PREV, Z_NEXT = range(4)
    near = (
        (lax.rem(t_place + t_count - 1, t_count), z_place),
        (lax.rem(t_place + 1, t_count), z_place),
        (t_place, lax.rem(z_place + z_count - 1, z_count)),
        (t_place, lax.rem(z_place + 1, z_count)),
    )
    first = (t_place > 0, t_place == t_count - 1, z_place > 0, z_place == z_count - 1)
    barrier = pltpu.get_barrier_semaphore()

    groups = [(x_hbm, psi_in)]
    for part in (pl.ds(36, 18), pl.ds(54, 18), pl.ds(0, 36)):
        groups.append((u_hbm.at[part], link_in.at[part]))
    groups.append((c_hbm, clov_in))

    def fetch(n):
        pltpu.make_async_copy(*groups[n], in_sem.at[n]).start()

    def arrived(n):
        pltpu.make_async_copy(*groups[n], in_sem.at[n]).wait()

    even = lax.rem(t_place, 2) == 0
    relay = jnp.logical_and(even, t_place > 0)
    t_after = near[T_NEXT][0]
    relayed = jnp.logical_and(lax.rem(t_after, 2) == 0, t_after > 0)
    z_low, z_high = z_place == 0, z_place == z_count - 1

    def greet(k, when):
        @pl.when(jnp.logical_and(when, jnp.logical_not(first[k])))
        def _():
            pl.semaphore_signal(barrier, inc=1, device_id=near[k], device_id_type=MESH)

    fetch(0)
    after = {Z_PREV: relay, T_PREV: jnp.logical_and(t_place == 0, z_place == 1)}
    for k in range(4):
        greet(k, jnp.logical_not(after[k]) if k in after else True)

    for n in (1, 2):
        fetch(n)
    greeters = sum(f.astype(jnp.int32) for f in first)

    @pl.when(greeters > 0)
    def _():
        pl.semaphore_wait(barrier, greeters)

    for k, when in after.items():
        greet(k, when)
    for k in range(4):
        @pl.when(first[k])
        def _():
            pl.semaphore_signal(ready.at[k ^ 1], inc=1, device_id=near[k], device_id_type=MESH)
    for n in (3, 4):
        fetch(n)

    def store_spinor(ref, at, value):
        for s in range(4):
            for c in range(3):
                ref[3 * s + c, at, :] = value[s][c][0]
                ref[12 + 3 * s + c, at, :] = value[s][c][1]

    def store_half(ref, mu, at, value):
        for s in range(2):
            for c in range(3):
                ref[mu, 3 * s + c, at, :] = value[s][c][0]
                ref[mu, 6 + 3 * s + c, at, :] = value[s][c][1]

    lane = lax.broadcasted_iota(jnp.int32, (rows, LANES), 1)
    row = lax.broadcasted_iota(jnp.int32, (rows, LANES), 0)
    lane_in = lax.rem(lane, NX)
    row_in = lax.rem(row, face_t)
    upper = lane >= NX

    def shift_x1(value, step):
        if step == 1:
            near, far = pltpu.roll(value, LANES - 1, 1), pltpu.roll(value, NX - 1, 1)
            return jnp.where(lane_in == NX - 1, far, near)
        near, far = pltpu.roll(value, 1, 1), pltpu.roll(value, LANES - NX + 1, 1)
        return jnp.where(lane_in == 0, far, near)

    def shift_x2(value, step):
        turned = pltpu.roll(value, NX, 1)
        if step == 1:
            near = pltpu.roll(turned, rows - nz, 0)
            far = pltpu.roll(turned, face_t - nz, 0)
            moved = jnp.where(row_in >= face_t - nz, far, near)
            return jnp.where(upper, moved, turned)
        near = pltpu.roll(turned, nz, 0)
        far = pltpu.roll(turned, rows - face_t + nz, 0)
        moved = jnp.where(row_in < nz, far, near)
        return jnp.where(upper, turned, moved)

    def z_ahead(src, dst, c):
        for z in range(nz - 1):
            dst[2, c, pl.ds(z, face_z, nz), :] = src[2, c, pl.ds(z + 1, face_z, nz), :]

    def z_behind(src, dst, c):
        for z in range(1, nz):
            dst[2, c, pl.ds(z, face_z, nz), :] = src[2, c, pl.ds(z - 1, face_z, nz), :]

    def t_ahead(src, dst, c):
        dst[3, c, pl.ds(0, rows - face_t), :] = src[3, c, pl.ds(face_t, rows - face_t), :]

    def t_behind(src, dst, c):
        dst[3, c, pl.ds(face_t, rows - face_t), :] = src[3, c, pl.ds(0, rows - face_t), :]

    t_last, z_last = nt - 1, nz - 1
    messages = {
        "a0": (T_PREV, [(0, 0)], [(t_last, 0)]),
        "a1": (T_PREV, [(0, z) for z in range(1, nz)], [(t_last, z) for z in range(1, nz)]),
        "b0": (T_NEXT, [(t_last, 0)], [(0, 0)]),
        "b1": (T_NEXT, [(t_last, z) for z in range(1, nz)], [(0, z) for z in range(1, nz)]),
        "c0": (Z_PREV, [(0, 0)], [(0, z_last)]),
        "c1": (Z_PREV, [(t, 0) for t in range(1, nt)], [(t, z_last) for t in range(1, nt)]),
        "d0": (Z_NEXT, [(0, z_last)], [(0, 0)]),
        "d1": (Z_NEXT, [(t, z_last) for t in range(1, nt)], [(t, 0) for t in range(1, nt)]),
        "e0": (Z_PREV, [(t, 0) for t in range(t_last)], [(t, z_last) for t in range(t_last)]),
        "e1": (Z_PREV, [(t_last, 0)], [(t_last, z_last)]),
        "f0": (T_PREV, [(0, z) for z in range(z_last)], [(t_last, z) for z in range(z_last)]),
        "f1": (T_PREV, [(0, z_last)], [(t_last, z_last)]),
    }
    names = list(messages)

    def place(name, i, c):
        return names.index(name), pl.ds((12 * i + c) * line, line)

    def lines(at):
        return pl.ds(at[0] * face_t + at[1], line, nz)

    def pack(name, src, mu):
        for i, at in enumerate(messages[name][1]):
            for c in range(12):
                k, held = place(name, i, c)
                face_out[k, held, :] = src[mu, c, lines(at), :]

    def unpack(name, dst, mu, change=lambda value, at, c: value):
        for i, at in enumerate(messages[name][2]):
            for c in range(12):
                k, held = place(name, i, c)
                dst[mu, c, lines(at), :] = change(face_in[k, held, :], at, c)

    together = ("a0", "b0", "c0", "d0", "a1 b1", "c1 d1", "e0 e1", "f0 f1")
    home = {name: n for n, some in enumerate(together) for name in some.split()}
    sizes = {name: 12 * line * len(messages[name][1]) for name in names}

    def copy_of(name):
        k, size = names.index(name), pl.ds(0, sizes[name])
        return pltpu.make_async_remote_copy(
            src_ref=face_out.at[k, size], dst_ref=face_in.at[k, size], send_sem=send_sem.at[0],
            recv_sem=recv_sem.at[home[name]], device_id=near[messages[name][0]], device_id_type=MESH,
        )

    copies = {name: copy_of(name) for name in names}

    def await_rows(count, sem):
        held = face_in.reshape(face_in.shape[0] * face_in.shape[1], LANES).at[pl.ds(0, count)]
        pltpu.make_async_copy(held, held, sem).wait()

    CORNER = len(together)

    def corner_of(k, held, target):
        size = pl.ds(0, held.shape[0])
        return pltpu.make_async_remote_copy(
            src_ref=held, dst_ref=corner_in.at[k, size], send_sem=send_sem.at[1],
            recv_sem=recv_sem.at[CORNER], device_id=target, device_id_type=MESH,
        )

    t_before = near[T_PREV][0]
    corners = [
        corner_of(0, face_out.at[names.index("d0"), pl.ds(0, 12 * line)], (t_before, near[Z_NEXT][1])),
        corner_of(1, face_out.at[names.index("c0"), pl.ds(0, 12 * line)], (t_before, near[Z_PREV][1])),
        corner_of(2, link_out, near[T_PREV]),
        corner_of(0, face_out.at[names.index("b0"), pl.ds(0, 12 * line)], (near[T_NEXT][0], near[Z_PREV][1])),
    ]
    edge = jnp.logical_and(t_place == 0, z_place == 1)
    edge_from = jnp.logical_and(t_place == t_count - 1, z_place == 1)
    edge_to = jnp.logical_and(t_place == 0, z_low)
    relay_high, relay_low = jnp.logical_and(relay, z_high), jnp.logical_and(relay, z_low)
    relayed_high, relayed_low = jnp.logical_and(relayed, z_high), jnp.logical_and(relayed, z_low)
    def sender(mine):
        greeted = set()

        def early(*some):
            for name in some:
                pl.when(jnp.logical_and(mine, first[messages[name][0]]))(copies[name].start)

        def late(*some):
            for name in some:
                side = messages[name][0]

                @pl.when(jnp.logical_and(mine, jnp.logical_not(first[side])))
                def _():
                    if side not in greeted:
                        pl.semaphore_wait(ready.at[side], 1)
                    copies[name].start()

                greeted.add(side)

        return early, late

    even_early, even_late = sender(even)
    odd_early, odd_late = sender(jnp.logical_not(even))

    def received(*some):
        assert set(some) == {name for name in names if home[name] == home[some[0]]}
        await_rows(sum(sizes[name] for name in some), recv_sem.at[home[some[0]]])

    def project(mu, v):
        at = window(v)
        field = load_spinor(psi, at)
        store_half(hm, mu, at, half(mu, field, -1.0))
        ahead = half(mu, field, 1.0)
        store_half(hp, mu, at, ahead)
        store_half(bl, mu, at, mat_vec(load_link(link, mu, at), ahead, True))

    inner = jnp.logical_not(first[Z_NEXT])
    arrived(0)
    for name in ("c0", "c1"):
        for i, at in enumerate(messages[name][1]):
            ahead = half(2, load_spinor(psi, lines(at)), -1.0)
            for c in range(12):
                k, spot = place(name, i, c)
                face_out[k, spot, :] = ahead[c % 6 // 3][c % 3][c // 6]
    for name in ("c0", "c1"):
        pl.when(jnp.logical_and(inner, first[Z_PREV]))(copies[name].start)
    arrived(1)
    for_each(chunks, lambda v: project(2, v))
    for name in ("d0", "d1"):
        pack(name, bl, 2)
    for some in (copies["c0"], corners[0], copies["d0"], copies["d1"]):
        pl.when(relay_high)(some.start)
    for name in ("d0", "d1", "c0"):
        pl.when(jnp.logical_and(z_high, t_place == 0))(copies[name].start)
    arrived(2)
    for_each(chunks, lambda v: project(3, v))
    for name in ("a0", "a1"):
        pack(name, hm, 3)
    for name in ("b0", "b1"):
        pack(name, bl, 3)
    even_early("b0", "a0", "a1", "b1")
    even_late("b0", "b1")
    pl.when(edge_from)(corners[3].start)
    odd_early("a0", "b0", "a1", "b1", "d0")
    for c in range(18):
        link_out[c * line:(c + 1) * line, :] = link[36 + c, lines((0, z_last)), :]
    pl.when(relay_high)(corners[2].start)
    pl.when(jnp.logical_and(even, z_high))(copies["c1"].start)
    pl.when(jnp.logical_and(jnp.logical_not(even), z_high))(copies["c0"].start)

    arrived(3)
    for_each(chunks, lambda v: project(0, v))
    for_each(chunks, lambda v: project(1, v))

    for c in range(12):
        sh_hm[0, c] = shift_x1(hm[0, c], 1)
        sh_bl[0, c] = shift_x1(bl[0, c], -1)
        sh_hm[1, c] = shift_x2(hm[1, c], 1)
        sh_bl[1, c] = shift_x2(bl[1, c], -1)
        z_ahead(hm, sh_hm, c)
        z_behind(bl, sh_bl, c)
        t_ahead(hm, sh_hm, c)
        t_behind(bl, sh_bl, c)

    def hop(mu, at, total):
        ahead = mat_vec(load_link(link, mu, at), load_half(sh_hm, mu, at), False)
        store_half(prod, mu, at, ahead)
        total = add_whole(mu, total, ahead, -1.0)
        return add_whole(mu, total, load_half(sh_bl, mu, at), 1.0)

    zero = jnp.zeros((TILE, LANES), jnp.float32)

    def nothing():
        return [[(zero, zero)] * 3 for _ in range(4)]

    even_late("d0", "d1")
    odd_late("d0", "d1")
    arrived(4)

    def local(v):
        at = window(v)
        field = load_spinor(psi, at)
        total = nothing()
        for mu in (0, 1):
            total = hop(mu, at, total)
        for s in range(4):
            for c in range(3):
                base = 36 * (s // 2) + 6 * (3 * (s % 2) + c)
                re = (4.0 + bare_mass) * field[s][c][0] - 0.5 * total[s][c][0]
                im = (4.0 + bare_mass) * field[s][c][1] - 0.5 * total[s][c][1]
                for k in range(6):
                    other = field[2 * (s // 2) + k // 3][k % 3]
                    c_re = clov[base + k, at, :]
                    c_im = clov[72 + base + k, at, :]
                    re = re + (c_re * other[0] - c_im * other[1])
                    im = im + (c_re * other[1] + c_im * other[0])
                acc[3 * s + c, at, :] = re
                acc[12 + 3 * s + c, at, :] = im

    for_each(chunks, local)

    def with_hops(mu, at):
        total = hop(mu, at, nothing())
        held = load_spinor(acc, at)
        return [
            [(held[s][c][0] - 0.5 * total[s][c][0], held[s][c][1] - 0.5 * total[s][c][1]) for c in range(3)]
            for s in range(4)
        ]

    def partial(across, along, v):
        at = window(v)
        store_half(hphi, along, at, half(along, with_hops(across, at), 1.0))

    def signed(sign):
        return lambda value, at, c: value * sign

    low_chunks = -(-face_t // TILE)
    high_chunk = (rows - face_t) // TILE

    odd_early("d1")
    pl.when(jnp.logical_and(jnp.logical_not(even), z_high))(copies["c1"].start)
    odd_late("b0", "b1")
    for c in range(12):
        sh_bl[2, c, lines((0, 0)), :] = jnp.zeros((line, LANES), jnp.float32)
        sh_hm[2, c, lines((0, z_last)), :] = jnp.zeros((line, LANES), jnp.float32)

    def send_f(name, when):
        @pl.when(when)
        def _():
            for_each(low_chunks, lambda v: partial(2, 3, v))
            pack(name, hphi, 3)
            copies[name].start()

    send_f("f0", relay_low)
    send_f("f1", relay_high)

    def wrap():
        copies["c0"].start()
        copies["c1"].start()

    @pl.when(z_low)
    def _():
        pl.semaphore_wait(ready.at[Z_PREV], 1)
        pl.when(relay)(corners[1].start)
        pl.when(jnp.logical_not(relayed))(wrap)

    even_late("a0", "a1")
    odd_late("a0", "a1")

    def send_e(name):
        low, high = (high_chunk, chunks) if name == "e1" else (0, -(-(rows - face_t) // TILE))
        for_each(high, lambda v: partial(3, 2, v), low)
        pack(name, hphi, 2)
        copies[name].start()

    def take_a():
        received("a0")
        unpack("a0", sh_hm, 3, signed(high_sign))
        send_e("e1")

    def take_b():
        received("b0")
        unpack("b0", sh_bl, 3, signed(low_sign))
        pl.when(jnp.logical_not(edge))(lambda: send_e("e0"))

    @pl.when(edge)
    def _():
        for c in range(12):
            sh_bl[3, c, lines((0, 0)), :] = jnp.zeros((line, LANES), jnp.float32)
        send_e("e0")

    pl.when(jnp.logical_not(even))(take_b)
    take_a()
    pl.when(even)(take_b)
    pl.when(jnp.logical_and(z_low, relayed))(wrap)

    def take_c():
        received("c0")
        unpack("c0", sh_hm, 2)
        send_f("f1", jnp.logical_not(relay_high))

    def take_d():
        received("d0")
        unpack("d0", sh_bl, 2)
        send_f("f0", jnp.logical_not(relay_low))

    pl.when(jnp.logical_not(z_low))(take_d)
    take_c()
    pl.when(z_low)(take_d)

    received("a1", "b1")
    unpack("a1", sh_hm, 3, signed(high_sign))
    unpack("b1", sh_bl, 3, signed(low_sign))

    def gather(v):
        at = window(v)
        store_spinor(acc, at, with_hops(3, at))

    for_each(chunks, gather)
    received("c1", "d1")
    unpack("c1", sh_hm, 2)
    unpack("d1", sh_bl, 2)

    def finish(v):
        at = window(v)
        phi = with_hops(2, at)
        store_spinor(out_ref, at, phi)
        for mu in range(4):
            store_half(hphi, mu, at, half(mu, phi, 1.0))

    for_each(chunks, finish)

    for c in range(12):
        sh_hphi[0, c] = shift_x1(hphi[0, c], 1)
        sh_hphi[1, c] = shift_x2(hphi[1, c], 1)
        z_ahead(hphi, sh_hphi, c)
        t_ahead(hphi, sh_hphi, c)

    for mu in (0, 1):
        for_each(chunks, lambda v: force_of(mu, v, out_ref, link, hp, prod, sh_hphi, force_ref, 18 * mu))

    received("f0", "f1")
    for name in ("f0", "f1"):
        unpack(name, sh_hphi, 3, lambda value, at, c: value * high_sign - bl[3, c, lines(at), :])

    @pl.when(edge_to)
    def _():
        for_each(chunks, lambda v: force_of(3, v, out_ref, link, hp, prod, sh_hphi, force_ref, 36))

    received("e0", "e1")
    for name in ("e0", "e1"):
        unpack(name, sh_hphi, 2, lambda value, at, c: value - bl[2, c, lines(at), :])

    def corner(k, c):
        return corner_in[k, c * line:(c + 1) * line, :]

    def corner_half(k):
        return [[(corner(k, 3 * s + c), corner(k, 6 + 3 * s + c)) for c in range(3)] for s in range(2)]

    none = [[(0.0, 0.0)] * 3 for _ in range(4)]

    def add_corner(across, along, value, sign, at, factor):
        extra = half(along, add_whole(across, none, value, sign), 1.0)
        for s in range(2):
            for c in range(3):
                for n, part in enumerate(extra[s][c]):
                    place = along, 6 * n + 3 * s + c, lines(at), slice(None)
                    sh_hphi[place] = sh_hphi[place] - 0.5 * factor * part

    @pl.when(relayed_low)
    def _():
        await_rows(12 * line, recv_sem.at[CORNER])
        add_corner(2, 3, corner_half(0), 1.0, (t_last, 0), high_sign)

    @pl.when(relayed_high)
    def _():
        await_rows(30 * line, recv_sem.at[CORNER])
        near_link = [[(corner(2, 3 * a + b), corner(2, 9 + 3 * a + b)) for b in range(3)] for a in range(3)]
        add_corner(2, 3, mat_vec(near_link, corner_half(1), False), -1.0, (t_last, z_last), high_sign)

    @pl.when(edge_to)
    def _():
        await_rows(12 * line, recv_sem.at[CORNER])
        add_corner(3, 2, corner_half(0), 1.0, (0, z_last), low_sign)

    await_rows(sum(sizes.values()), send_sem.at[0])
    for mine, count in ((relay_high, 30), (jnp.logical_or(relay_low, edge_from), 12)):
        pl.when(mine)(lambda: await_rows(count * line, send_sem.at[1]))


def body(spinor, links, clover):
    nt, nz, plane = spinor.shape[-3:]
    pieces = plane // LANES

    def tiled(a):
        return a.reshape(-1, nt, nz, pieces, LANES).transpose(0, 1, 3, 2, 4)

    def untiled(a, shape):
        return a.transpose(0, 1, 3, 2, 4).reshape(shape)

    x, u, c = map(tiled, (spinor, links, clover))
    rows = nt * pieces * nz
    assert nt > 1 and nz > 1
    line = rows // (nt * nz)
    face = max(nt - 1, nz - 1) * line

    def halves():
        return pltpu.VMEM((4, 12, rows, LANES), jnp.float32)

    def held(array):
        return pltpu.VMEM(array.shape, jnp.float32)

    made = pl.pallas_call(
        lambda *refs: kernel(nt, nz, *refs),
        name="wilson",
        out_shape=(held(x), held(u[:54]), held(u), halves(), halves(), halves()),
        in_specs=[pl.BlockSpec(memory_space=pltpu.HBM)] * 3,
        out_specs=(pl.BlockSpec(memory_space=pltpu.VMEM),) * 6,
        scratch_shapes=[
            held(x), held(c),
            halves(), halves(), halves(), halves(),
            pltpu.VMEM((24, rows, LANES), jnp.float32),
            halves(),
            pltpu.VMEM((12, 12 * face, LANES), jnp.float32),
            pltpu.VMEM((12, 12 * face, LANES), jnp.float32),
            pltpu.VMEM((18 * line, LANES), jnp.float32),
            pltpu.VMEM((3, 18 * line, LANES), jnp.float32),
            pltpu.SemaphoreType.DMA((5,)),
            pltpu.SemaphoreType.DMA((2,)),
            pltpu.SemaphoreType.DMA((9,)),
            pltpu.SemaphoreType.REGULAR((4,)),
        ],
        compiler_params=pltpu.CompilerParams(
            collective_id=0, has_side_effects=True, vmem_limit_bytes=54 * 1024 * 1024
        ),
    )(x, u, c)
    applied, force = pl.pallas_call(
        finish_kernel,
        name="finish",
        out_shape=(
            jax.ShapeDtypeStruct(x.shape, jnp.float32),
            jax.ShapeDtypeStruct(u.shape, jnp.float32),
        ),
        in_specs=[pl.BlockSpec(memory_space=pltpu.VMEM)] * 6,
        out_specs=(pl.BlockSpec(memory_space=pl.ANY),) * 2,
        scratch_shapes=[held(u[:36]), pltpu.SemaphoreType.DMA((2,))],
        compiler_params=pltpu.CompilerParams(vmem_limit_bytes=8 * 1024 * 1024),
    )(*made)
    return untiled(applied, spinor.shape), untiled(force, links.shape)


def solution(mesh):
    return jax.shard_map(
        body,
        mesh=mesh,
        in_specs=(
            P(None, None, None, "ta", "gz", None),
            P(None, None, None, None, "ta", "gz", None),
            P(None, None, None, None, "ta", "gz", None),
        ),
        out_specs=(
            P(None, None, None, "ta", "gz", None),
            P(None, None, None, None, "ta", "gz", None),
        ),
        check_vma=False,
    )
```

```python
import jax
import jax.numpy as jnp
from jax import lax
from jax.experimental import pallas as pl
from jax.experimental.pallas import tpu as pltpu
from jax.sharding import PartitionSpec as P

NX = 64
LANES = 128
TILE = 8
MESH = pl.DeviceIdType.MESH

bare_mass = -0.25
gamma_table = (
    ((3, 0.0, -1.0), (2, 0.0, -1.0), (1, 0.0, 1.0), (0, 0.0, 1.0)),
    ((3, -1.0, 0.0), (2, 1.0, 0.0), (1, 1.0, 0.0), (0, -1.0, 0.0)),
    ((2, 0.0, -1.0), (3, 0.0, 1.0), (0, 0.0, 1.0), (1, 0.0, -1.0)),
    ((2, 1.0, 0.0), (3, 1.0, 0.0), (0, 1.0, 0.0), (1, 1.0, 0.0)),
)


def add_signed(a, b, positive):
    return a + b if positive else a - b


def add_phase(a, b, phase_re, phase_im):
    if phase_im == 0.0:
        up = phase_re > 0
        return (add_signed(a[0], b[0], up), add_signed(a[1], b[1], up))
    up = phase_im > 0
    return (add_signed(a[0], b[1], not up), add_signed(a[1], b[0], up))


def half(mu, field, sign):
    out = []
    for s in range(2):
        source, p_re, p_im = gamma_table[mu][s]
        out.append(
            [add_phase(field[s][c], field[source][c], sign * p_re, sign * p_im) for c in range(3)]
        )
    return out


def add_whole(mu, total, halves, sign):
    out = [[add_phase(total[s][c], halves[s][c], 1.0, 0.0) for c in range(3)] for s in range(2)]
    for s in (2, 3):
        source, p_re, p_im = gamma_table[mu][s]
        out.append(
            [add_phase(total[s][c], halves[source][c], sign * p_re, sign * p_im) for c in range(3)]
        )
    return out


def csum(terms):
    total = terms[0]
    for term in terms[1:]:
        total = total + term
    return total


def mat_vec(link, vec, dagger):
    out = []
    for s in range(2):
        rows = []
        for a in range(3):
            re, im = [], []
            for b in range(3):
                h = vec[s][b]
                if dagger:
                    m = link[b][a]
                    re.append(m[0] * h[0] + m[1] * h[1])
                    im.append(m[0] * h[1] - m[1] * h[0])
                else:
                    m = link[a][b]
                    re.append(m[0] * h[0] - m[1] * h[1])
                    im.append(m[0] * h[1] + m[1] * h[0])
            rows.append((csum(re), csum(im)))
        out.append(rows)
    return out


def flat(ref):
    return ref.reshape(ref.shape[0], ref.shape[1] * ref.shape[2] * ref.shape[3], ref.shape[4])


def for_each(count, body, low=0):
    def step(i, carry):
        body(i)
        return carry

    lax.fori_loop(low, count, step, 0)


def window(v):
    return pl.ds(pl.multiple_of(v * TILE, TILE), TILE)


def load_spinor(ref, at):
    return [[(ref[3 * s + c, at, :], ref[12 + 3 * s + c, at, :]) for c in range(3)] for s in range(4)]


def load_half(ref, mu, at):
    return [[(ref[mu, 3 * s + c, at, :], ref[mu, 6 + 3 * s + c, at, :]) for c in range(3)] for s in range(2)]


def load_link(ref, mu, at):
    return [[(ref[18 * mu + 3 * a + b, at, :], ref[18 * mu + 9 + 3 * a + b, at, :]) for b in range(3)] for a in range(3)]


def force_of(mu, v, phi, link, hp, prod, hphi, force_ref, base):
    at = window(v)
    zero = jnp.zeros((TILE, LANES), jnp.float32)
    second = mat_vec(load_link(link, mu, at), load_half(hphi, mu, at), False)
    second_right = load_half(hp, mu, at)
    first = load_half(prod, mu, at)
    first_right = half(mu, load_spinor(phi, at), -1.0)
    pairs = [(first[s], first_right[s]) for s in range(2)] + [(second[s], second_right[s]) for s in range(2)]

    def w_re(a, b):
        return csum([l[a][0] * r[b][0] + l[a][1] * r[b][1] for l, r in pairs])

    def w_im(a, b):
        return csum([l[a][1] * r[b][0] - l[a][0] * r[b][1] for l, r in pairs])

    diag = [w_im(a, a) for a in range(3)]
    third = (diag[0] + diag[1] + diag[2]) * (1.0 / 3.0)
    for a in range(3):
        force_ref[base + 4 * a, at, :] = zero
        force_ref[base + 9 + 4 * a, at, :] = diag[a] - third
        for b in range(a + 1, 3):
            re = 0.5 * (w_re(a, b) - w_re(b, a))
            im = 0.5 * (w_im(a, b) + w_im(b, a))
            force_ref[base + 3 * a + b, at, :] = re
            force_ref[base + 3 * b + a, at, :] = -re
            force_ref[base + 9 + 3 * a + b, at, :] = im
            force_ref[base + 9 + 3 * b + a, at, :] = im


def finish_kernel(phi_in, early_in, link_in, hp, prod, hphi, phi_hbm, force_hbm, late, sem):
    phi, link = flat(phi_in), flat(link_in)
    corner = jnp.logical_and(lax.axis_index("ta") == 0, lax.axis_index("gz") == 0)

    def write(held, mu, count=1):
        pltpu.make_async_copy(held, force_hbm.at[pl.ds(18 * mu, 18 * count)], sem.at[0]).start()

    def compute(mu, base):
        for_each(
            phi.shape[1] // TILE, lambda v: force_of(mu, v, phi, link, hp, prod, hphi, flat(late), base)
        )
        write(late.at[pl.ds(base, 18)], mu)

    write(early_in.at[pl.ds(0, 36)], 0, 2)
    applied = pltpu.make_async_copy(phi_in, phi_hbm, sem.at[1])
    applied.start()
    pl.when(corner)(lambda: write(early_in.at[pl.ds(36, 18)], 3))
    pl.when(jnp.logical_not(corner))(lambda: compute(3, 18))
    compute(2, 0)
    applied.wait()
    pltpu.make_async_copy(force_hbm, force_hbm, sem.at[0]).wait()


def kernel(nt, nz, x_hbm, u_hbm, c_hbm, phi_out, force_out, link_in, hp, prod, sh_hphi, psi_in, clov_in, hm, bl,
           sh_hm, sh_bl, acc, hphi, face_out, face_in, link_out, corner_in, in_sem,
           send_sem, recv_sem, ready):
    psi, link, clov, out_ref, force_ref = map(flat, (psi_in, link_in, clov_in, phi_out, force_out))
    rows = psi.shape[1]
    face_t = rows // nt
    face_z = rows // nz
    line = face_t // nz
    chunks = rows // TILE
    t_place, z_place = lax.axis_index("ta"), lax.axis_index("gz")
    t_count, z_count = lax.axis_size("ta"), lax.axis_size("gz")
    low_sign = jnp.where(t_place == 0, -1.0, 1.0).astype(jnp.float32)
    high_sign = jnp.where(t_place == t_count - 1, -1.0, 1.0).astype(jnp.float32)

    T_PREV, T_NEXT, Z_PREV, Z_NEXT = range(4)
    near = (
        (lax.rem(t_place + t_count - 1, t_count), z_place),
        (lax.rem(t_place + 1, t_count), z_place),
        (t_place, lax.rem(z_place + z_count - 1, z_count)),
        (t_place, lax.rem(z_place + 1, z_count)),
    )
    first = (t_place > 0, t_place == t_count - 1, z_place > 0, z_place == z_count - 1)
    barrier = pltpu.get_barrier_semaphore()

    groups = [(x_hbm, psi_in)]
    for part in (pl.ds(36, 36), pl.ds(0, 36)):
        groups.append((u_hbm.at[part], link_in.at[part]))
    groups.append((c_hbm, clov_in))

    def fetch(n):
        pltpu.make_async_copy(*groups[n], in_sem.at[n]).start()

    def arrived(n):
        pltpu.make_async_copy(*groups[n], in_sem.at[n]).wait()

    even = lax.rem(t_place, 2) == 0
    relay = jnp.logical_and(even, t_place > 0)
    t_after = near[T_NEXT][0]
    relayed = jnp.logical_and(lax.rem(t_after, 2) == 0, t_after > 0)
    z_low, z_high = z_place == 0, z_place == z_count - 1

    def greet(k, when):
        @pl.when(jnp.logical_and(when, jnp.logical_not(first[k])))
        def _():
            pl.semaphore_signal(barrier, inc=1, device_id=near[k], device_id_type=MESH)

    fetch(0)
    after = {Z_PREV: relay, T_PREV: jnp.logical_and(t_place == 0, z_place == 1)}
    for k in range(4):
        greet(k, jnp.logical_not(after[k]) if k in after else True)

    fetch(1)
    greeters = sum(f.astype(jnp.int32) for f in first)

    @pl.when(greeters > 0)
    def _():
        pl.semaphore_wait(barrier, greeters)

    for k, when in after.items():
        greet(k, when)
    for k in range(4):
        @pl.when(first[k])
        def _():
            pl.semaphore_signal(ready.at[k ^ 1], inc=1, device_id=near[k], device_id_type=MESH)
    for n in (2, 3):
        fetch(n)

    def store_spinor(ref, at, value):
        for s in range(4):
            for c in range(3):
                ref[3 * s + c, at, :] = value[s][c][0]
                ref[12 + 3 * s + c, at, :] = value[s][c][1]

    def store_half(ref, mu, at, value):
        for s in range(2):
            for c in range(3):
                ref[mu, 3 * s + c, at, :] = value[s][c][0]
                ref[mu, 6 + 3 * s + c, at, :] = value[s][c][1]

    lane = lax.broadcasted_iota(jnp.int32, (rows, LANES), 1)
    row = lax.broadcasted_iota(jnp.int32, (rows, LANES), 0)
    lane_in = lax.rem(lane, NX)
    row_in = lax.rem(row, face_t)
    upper = lane >= NX

    def shift_x1(value, step):
        if step == 1:
            near, far = pltpu.roll(value, LANES - 1, 1), pltpu.roll(value, NX - 1, 1)
            return jnp.where(lane_in == NX - 1, far, near)
        near, far = pltpu.roll(value, 1, 1), pltpu.roll(value, LANES - NX + 1, 1)
        return jnp.where(lane_in == 0, far, near)

    def shift_x2(value, step):
        turned = pltpu.roll(value, NX, 1)
        if step == 1:
            near = pltpu.roll(turned, rows - nz, 0)
            far = pltpu.roll(turned, face_t - nz, 0)
            moved = jnp.where(row_in >= face_t - nz, far, near)
            return jnp.where(upper, moved, turned)
        near = pltpu.roll(turned, nz, 0)
        far = pltpu.roll(turned, rows - face_t + nz, 0)
        moved = jnp.where(row_in < nz, far, near)
        return jnp.where(upper, turned, moved)

    def z_ahead(src, dst, c):
        for z in range(nz - 1):
            dst[2, c, pl.ds(z, face_z, nz), :] = src[2, c, pl.ds(z + 1, face_z, nz), :]

    def z_behind(src, dst, c):
        for z in range(1, nz):
            dst[2, c, pl.ds(z, face_z, nz), :] = src[2, c, pl.ds(z - 1, face_z, nz), :]

    def t_ahead(src, dst, c):
        dst[3, c, pl.ds(0, rows - face_t), :] = src[3, c, pl.ds(face_t, rows - face_t), :]

    def t_behind(src, dst, c):
        dst[3, c, pl.ds(face_t, rows - face_t), :] = src[3, c, pl.ds(0, rows - face_t), :]

    t_last, z_last = nt - 1, nz - 1
    messages = {
        "a0": (T_PREV, [(0, 0)], [(t_last, 0)]),
        "a1": (T_PREV, [(0, z) for z in range(1, nz)], [(t_last, z) for z in range(1, nz)]),
        "b0": (T_NEXT, [(t_last, 0)], [(0, 0)]),
        "b1": (T_NEXT, [(t_last, z) for z in range(1, nz)], [(0, z) for z in range(1, nz)]),
        "c0": (Z_PREV, [(0, 0)], [(0, z_last)]),
        "c1": (Z_PREV, [(t, 0) for t in range(1, nt)], [(t, z_last) for t in range(1, nt)]),
        "d0": (Z_NEXT, [(0, z_last)], [(0, 0)]),
        "d1": (Z_NEXT, [(t, z_last) for t in range(1, nt)], [(t, 0) for t in range(1, nt)]),
        "e0": (Z_PREV, [(t, 0) for t in range(t_last)], [(t, z_last) for t in range(t_last)]),
        "e1": (Z_PREV, [(t_last, 0)], [(t_last, z_last)]),
        "f0": (T_PREV, [(0, z) for z in range(z_last)], [(t_last, z) for z in range(z_last)]),
        "f1": (T_PREV, [(0, z_last)], [(t_last, z_last)]),
    }
    names = list(messages)

    def place(name, i, c):
        return names.index(name), pl.ds((12 * i + c) * line, line)

    def lines(at):
        return pl.ds(at[0] * face_t + at[1], line, nz)

    def pack(name, src, mu):
        for i, at in enumerate(messages[name][1]):
            for c in range(12):
                k, held = place(name, i, c)
                face_out[k, held, :] = src[mu, c, lines(at), :]

    def unpack(name, dst, mu, change=lambda value, at, c: value):
        for i, at in enumerate(messages[name][2]):
            for c in range(12):
                k, held = place(name, i, c)
                dst[mu, c, lines(at), :] = change(face_in[k, held, :], at, c)

    together = ("a0", "b0", "c0", "d0", "a1 b1", "c1 d1", "e0 e1", "f0 f1")
    home = {name: n for n, some in enumerate(together) for name in some.split()}
    sizes = {name: 12 * line * len(messages[name][1]) for name in names}

    def copy_of(name):
        k, size = names.index(name), pl.ds(0, sizes[name])
        return pltpu.make_async_remote_copy(
            src_ref=face_out.at[k, size], dst_ref=face_in.at[k, size], send_sem=send_sem.at[0],
            recv_sem=recv_sem.at[home[name]], device_id=near[messages[name][0]], device_id_type=MESH,
        )

    copies = {name: copy_of(name) for name in names}

    def await_rows(count, sem):
        held = face_in.reshape(face_in.shape[0] * face_in.shape[1], LANES).at[pl.ds(0, count)]
        pltpu.make_async_copy(held, held, sem).wait()

    CORNER = len(together)

    def corner_of(k, held, target):
        size = pl.ds(0, held.shape[0])
        return pltpu.make_async_remote_copy(
            src_ref=held, dst_ref=corner_in.at[k, size], send_sem=send_sem.at[1],
            recv_sem=recv_sem.at[CORNER], device_id=target, device_id_type=MESH,
        )

    t_before = near[T_PREV][0]
    corners = [
        corner_of(0, face_out.at[names.index("d0"), pl.ds(0, 12 * line)], (t_before, near[Z_NEXT][1])),
        corner_of(1, face_out.at[names.index("c0"), pl.ds(0, 12 * line)], (t_before, near[Z_PREV][1])),
        corner_of(2, link_out, near[T_PREV]),
        corner_of(0, face_out.at[names.index("b0"), pl.ds(0, 12 * line)], (near[T_NEXT][0], near[Z_PREV][1])),
    ]
    edge = jnp.logical_and(t_place == 0, z_place == 1)
    edge_from = jnp.logical_and(t_place == t_count - 1, z_place == 1)
    edge_to = jnp.logical_and(t_place == 0, z_low)
    relay_high, relay_low = jnp.logical_and(relay, z_high), jnp.logical_and(relay, z_low)
    relayed_high, relayed_low = jnp.logical_and(relayed, z_high), jnp.logical_and(relayed, z_low)
    def sender(mine):
        greeted = set()

        def early(*some):
            for name in some:
                pl.when(jnp.logical_and(mine, first[messages[name][0]]))(copies[name].start)

        def late(*some):
            for name in some:
                side = messages[name][0]

                @pl.when(jnp.logical_and(mine, jnp.logical_not(first[side])))
                def _():
                    if side not in greeted:
                        pl.semaphore_wait(ready.at[side], 1)
                    copies[name].start()

                greeted.add(side)

        return early, late

    even_early, even_late = sender(even)
    odd_early, odd_late = sender(jnp.logical_not(even))

    def received(*some):
        assert set(some) == {name for name in names if home[name] == home[some[0]]}
        await_rows(sum(sizes[name] for name in some), recv_sem.at[home[some[0]]])

    def project(mu, v):
        at = window(v)
        field = load_spinor(psi, at)
        store_half(hm, mu, at, half(mu, field, -1.0))
        ahead = half(mu, field, 1.0)
        store_half(hp, mu, at, ahead)
        store_half(bl, mu, at, mat_vec(load_link(link, mu, at), ahead, True))

    inner = jnp.logical_not(first[Z_NEXT])
    arrived(0)
    for name in ("c0", "c1"):
        for i, at in enumerate(messages[name][1]):
            ahead = half(2, load_spinor(psi, lines(at)), -1.0)
            for c in range(12):
                k, spot = place(name, i, c)
                face_out[k, spot, :] = ahead[c % 6 // 3][c % 3][c // 6]
    for name in ("c0", "c1"):
        pl.when(jnp.logical_and(inner, first[Z_PREV]))(copies[name].start)
    arrived(1)
    for_each(chunks, lambda v: project(2, v))
    for name in ("d0", "d1"):
        pack(name, bl, 2)
    for some in (copies["c0"], corners[0], copies["d0"], copies["d1"]):
        pl.when(relay_high)(some.start)
    for name in ("d0", "d1", "c0"):
        pl.when(jnp.logical_and(z_high, t_place == 0))(copies[name].start)
    for_each(chunks, lambda v: project(3, v))
    for name in ("a0", "a1"):
        pack(name, hm, 3)
    for name in ("b0", "b1"):
        pack(name, bl, 3)
    even_early("b0", "a0", "a1", "b1")
    even_late("b0", "b1")
    pl.when(edge_from)(corners[3].start)
    odd_early("a0", "b0", "a1", "b1", "d0")
    for c in range(18):
        link_out[c * line:(c + 1) * line, :] = link[36 + c, lines((0, z_last)), :]
    pl.when(relay_high)(corners[2].start)
    pl.when(jnp.logical_and(even, z_high))(copies["c1"].start)
    pl.when(jnp.logical_and(jnp.logical_not(even), z_high))(copies["c0"].start)

    arrived(2)
    for_each(chunks, lambda v: project(0, v))
    for_each(chunks, lambda v: project(1, v))

    for c in range(12):
        sh_hm[0, c] = shift_x1(hm[0, c], 1)
        sh_bl[0, c] = shift_x1(bl[0, c], -1)
        sh_hm[1, c] = shift_x2(hm[1, c], 1)
        sh_bl[1, c] = shift_x2(bl[1, c], -1)
        z_ahead(hm, sh_hm, c)
        z_behind(bl, sh_bl, c)
        t_ahead(hm, sh_hm, c)
        t_behind(bl, sh_bl, c)

    def hop(mu, at, total):
        ahead = mat_vec(load_link(link, mu, at), load_half(sh_hm, mu, at), False)
        store_half(prod, mu, at, ahead)
        total = add_whole(mu, total, ahead, -1.0)
        return add_whole(mu, total, load_half(sh_bl, mu, at), 1.0)

    zero = jnp.zeros((TILE, LANES), jnp.float32)

    def nothing():
        return [[(zero, zero)] * 3 for _ in range(4)]

    even_late("d0", "d1")
    odd_late("d0", "d1")
    arrived(3)

    def local(v):
        at = window(v)
        field = load_spinor(psi, at)
        total = nothing()
        for mu in (0, 1):
            total = hop(mu, at, total)
        for s in range(4):
            for c in range(3):
                base = 36 * (s // 2) + 6 * (3 * (s % 2) + c)
                re = (4.0 + bare_mass) * field[s][c][0] - 0.5 * total[s][c][0]
                im = (4.0 + bare_mass) * field[s][c][1] - 0.5 * total[s][c][1]
                for k in range(6):
                    other = field[2 * (s // 2) + k // 3][k % 3]
                    c_re = clov[base + k, at, :]
                    c_im = clov[72 + base + k, at, :]
                    re = re + (c_re * other[0] - c_im * other[1])
                    im = im + (c_re * other[1] + c_im * other[0])
                acc[3 * s + c, at, :] = re
                acc[12 + 3 * s + c, at, :] = im

    for_each(chunks, local)

    def with_hops(mu, at):
        total = hop(mu, at, nothing())
        held = load_spinor(acc, at)
        return [
            [(held[s][c][0] - 0.5 * total[s][c][0], held[s][c][1] - 0.5 * total[s][c][1]) for c in range(3)]
            for s in range(4)
        ]

    def partial(across, along, v):
        at = window(v)
        store_half(hphi, along, at, half(along, with_hops(across, at), 1.0))

    def signed(sign):
        return lambda value, at, c: value * sign

    low_chunks = -(-face_t // TILE)
    high_chunk = (rows - face_t) // TILE

    odd_early("d1")
    pl.when(jnp.logical_and(jnp.logical_not(even), z_high))(copies["c1"].start)
    odd_late("b0", "b1")
    for c in range(12):
        sh_bl[2, c, lines((0, 0)), :] = jnp.zeros((line, LANES), jnp.float32)
        sh_hm[2, c, lines((0, z_last)), :] = jnp.zeros((line, LANES), jnp.float32)

    def send_f(name, when):
        @pl.when(when)
        def _():
            for_each(low_chunks, lambda v: partial(2, 3, v))
            pack(name, hphi, 3)
            copies[name].start()

    send_f("f0", relay_low)
    send_f("f1", relay_high)

    def wrap():
        copies["c0"].start()
        copies["c1"].start()

    @pl.when(z_low)
    def _():
        pl.semaphore_wait(ready.at[Z_PREV], 1)
        pl.when(relay)(corners[1].start)
        pl.when(jnp.logical_not(relayed))(wrap)

    even_late("a0", "a1")
    odd_late("a0", "a1")

    def send_e(name):
        low, high = (high_chunk, chunks) if name == "e1" else (0, -(-(rows - face_t) // TILE))
        for_each(high, lambda v: partial(3, 2, v), low)
        pack(name, hphi, 2)
        copies[name].start()

    def take_a():
        received("a0")
        unpack("a0", sh_hm, 3, signed(high_sign))
        send_e("e1")

    def take_b():
        received("b0")
        unpack("b0", sh_bl, 3, signed(low_sign))
        pl.when(jnp.logical_not(edge))(lambda: send_e("e0"))

    @pl.when(edge)
    def _():
        for c in range(12):
            sh_bl[3, c, lines((0, 0)), :] = jnp.zeros((line, LANES), jnp.float32)
        send_e("e0")

    pl.when(jnp.logical_not(even))(take_b)
    take_a()
    pl.when(even)(take_b)
    pl.when(jnp.logical_and(z_low, relayed))(wrap)

    def take_c():
        received("c0")
        unpack("c0", sh_hm, 2)
        send_f("f1", jnp.logical_not(relay_high))

    def take_d():
        received("d0")
        unpack("d0", sh_bl, 2)
        send_f("f0", jnp.logical_not(relay_low))

    pl.when(jnp.logical_not(z_low))(take_d)
    take_c()
    pl.when(z_low)(take_d)

    received("a1", "b1")
    unpack("a1", sh_hm, 3, signed(high_sign))
    unpack("b1", sh_bl, 3, signed(low_sign))

    def gather(v):
        at = window(v)
        store_spinor(acc, at, with_hops(3, at))

    for_each(chunks, gather)
    received("c1", "d1")
    unpack("c1", sh_hm, 2)
    unpack("d1", sh_bl, 2)

    def finish(v):
        at = window(v)
        phi = with_hops(2, at)
        store_spinor(out_ref, at, phi)
        for mu in range(4):
            store_half(hphi, mu, at, half(mu, phi, 1.0))

    for_each(chunks, finish)

    for c in range(12):
        sh_hphi[0, c] = shift_x1(hphi[0, c], 1)
        sh_hphi[1, c] = shift_x2(hphi[1, c], 1)
        z_ahead(hphi, sh_hphi, c)
        t_ahead(hphi, sh_hphi, c)

    for mu in (0, 1):
        for_each(chunks, lambda v: force_of(mu, v, out_ref, link, hp, prod, sh_hphi, force_ref, 18 * mu))

    received("f0", "f1")
    for name in ("f0", "f1"):
        unpack(name, sh_hphi, 3, lambda value, at, c: value * high_sign - bl[3, c, lines(at), :])

    @pl.when(edge_to)
    def _():
        for_each(chunks, lambda v: force_of(3, v, out_ref, link, hp, prod, sh_hphi, force_ref, 36))

    received("e0", "e1")
    for name in ("e0", "e1"):
        unpack(name, sh_hphi, 2, lambda value, at, c: value - bl[2, c, lines(at), :])

    def corner(k, c):
        return corner_in[k, c * line:(c + 1) * line, :]

    def corner_half(k):
        return [[(corner(k, 3 * s + c), corner(k, 6 + 3 * s + c)) for c in range(3)] for s in range(2)]

    none = [[(0.0, 0.0)] * 3 for _ in range(4)]

    def add_corner(across, along, value, sign, at, factor):
        extra = half(along, add_whole(across, none, value, sign), 1.0)
        for s in range(2):
            for c in range(3):
                for n, part in enumerate(extra[s][c]):
                    place = along, 6 * n + 3 * s + c, lines(at), slice(None)
                    sh_hphi[place] = sh_hphi[place] - 0.5 * factor * part

    @pl.when(relayed_low)
    def _():
        await_rows(12 * line, recv_sem.at[CORNER])
        add_corner(2, 3, corner_half(0), 1.0, (t_last, 0), high_sign)

    @pl.when(relayed_high)
    def _():
        await_rows(30 * line, recv_sem.at[CORNER])
        near_link = [[(corner(2, 3 * a + b), corner(2, 9 + 3 * a + b)) for b in range(3)] for a in range(3)]
        add_corner(2, 3, mat_vec(near_link, corner_half(1), False), -1.0, (t_last, z_last), high_sign)

    @pl.when(edge_to)
    def _():
        await_rows(12 * line, recv_sem.at[CORNER])
        add_corner(3, 2, corner_half(0), 1.0, (0, z_last), low_sign)

    await_rows(sum(sizes.values()), send_sem.at[0])
    for mine, count in ((relay_high, 30), (jnp.logical_or(relay_low, edge_from), 12)):
        pl.when(mine)(lambda: await_rows(count * line, send_sem.at[1]))


def body(spinor, links, clover):
    nt, nz, plane = spinor.shape[-3:]
    pieces = plane // LANES

    def tiled(a):
        return a.reshape(-1, nt, nz, pieces, LANES).transpose(0, 1, 3, 2, 4)

    def untiled(a, shape):
        return a.transpose(0, 1, 3, 2, 4).reshape(shape)

    x, u, c = map(tiled, (spinor, links, clover))
    rows = nt * pieces * nz
    assert nt > 1 and nz > 1
    line = rows // (nt * nz)
    face = max(nt - 1, nz - 1) * line

    def halves():
        return pltpu.VMEM((4, 12, rows, LANES), jnp.float32)

    def held(array):
        return pltpu.VMEM(array.shape, jnp.float32)

    made = pl.pallas_call(
        lambda *refs: kernel(nt, nz, *refs),
        name="wilson",
        out_shape=(held(x), held(u[:54]), held(u), halves(), halves(), halves()),
        in_specs=[pl.BlockSpec(memory_space=pltpu.HBM)] * 3,
        out_specs=(pl.BlockSpec(memory_space=pltpu.VMEM),) * 6,
        scratch_shapes=[
            held(x), held(c),
            halves(), halves(), halves(), halves(),
            pltpu.VMEM((24, rows, LANES), jnp.float32),
            halves(),
            pltpu.VMEM((12, 12 * face, LANES), jnp.float32),
            pltpu.VMEM((12, 12 * face, LANES), jnp.float32),
            pltpu.VMEM((18 * line, LANES), jnp.float32),
            pltpu.VMEM((3, 18 * line, LANES), jnp.float32),
            pltpu.SemaphoreType.DMA((4,)),
            pltpu.SemaphoreType.DMA((2,)),
            pltpu.SemaphoreType.DMA((9,)),
            pltpu.SemaphoreType.REGULAR((4,)),
        ],
        compiler_params=pltpu.CompilerParams(
            collective_id=0, has_side_effects=True, vmem_limit_bytes=54 * 1024 * 1024
        ),
    )(x, u, c)
    applied, force = pl.pallas_call(
        finish_kernel,
        name="finish",
        out_shape=(
            jax.ShapeDtypeStruct(x.shape, jnp.float32),
            jax.ShapeDtypeStruct(u.shape, jnp.float32),
        ),
        in_specs=[pl.BlockSpec(memory_space=pltpu.VMEM)] * 6,
        out_specs=(pl.BlockSpec(memory_space=pl.ANY),) * 2,
        scratch_shapes=[held(u[:36]), pltpu.SemaphoreType.DMA((2,))],
        compiler_params=pltpu.CompilerParams(vmem_limit_bytes=8 * 1024 * 1024),
    )(*made)
    return untiled(applied, spinor.shape), untiled(force, links.shape)


def solution(mesh):
    return jax.shard_map(
        body,
        mesh=mesh,
        in_specs=(
            P(None, None, None, "ta", "gz", None),
            P(None, None, None, None, "ta", "gz", None),
            P(None, None, None, None, "ta", "gz", None),
        ),
        out_specs=(
            P(None, None, None, "ta", "gz", None),
            P(None, None, None, None, "ta", "gz", None),
        ),
        check_vma=False,
    )
```
